32 devices in a mesh: dp: 4 (over y, z), ep: 8 (over x, core).
Axes of the slice: x: 4, y: 2, z: 2, core: 2. Of those that a mesh axis runs over, the one named last changes fastest.
The devices are a block of a 4x4x8 slice.
Arguments:
- hidden: bfloat16 [4096, 4096], P(('dp', 'ep')), parts along dimension 0
- k_cache: bfloat16 [4096, 32, 8, 128], P(('dp', 'ep')), parts along dimension 0
- v_cache: bfloat16 [4096, 32, 8, 128], P(('dp', 'ep')), parts along dimension 0
- seq_lens: int32 [4096], P(('dp', 'ep')), parts along dimension 0
- expert_ids: int32 [4096, 2], P(('dp', 'ep')), parts along dimension 0
- attn_gain: bfloat16 [4096], replicated
- w_query: bfloat16 [4096, 4096], replicated
- w_key: bfloat16 [4096, 1024], replicated
- w_value: bfloat16 [4096, 1024], replicated
- w_out: bfloat16 [4096, 4096], replicated
- ffn_gain: bfloat16 [4096], replicated
- w_router: bfloat16 [4096, 16], replicated
- w_gate: bfloat16 [16, 4096, 960], P('ep')
- w_up: bfloat16 [16, 4096, 960], P('ep')
- w_down: bfloat16 [16, 960, 4096], P('ep')
Outputs:
- output 1: bfloat16 [4096, 4096], P(('dp', 'ep')), parts along dimension 0
- output 2: bfloat16 [4096, 32, 8, 128], P(('dp', 'ep')), parts along dimension 0
- output 3: bfloat16 [4096, 32, 8, 128], P(('dp', 'ep')), parts along dimension 0
There are 4 independent parts. The reference program is written for one: setup_inputs(seed, part) draws one part's arguments, and reference() takes and returns one part's arrays. A program takes and returns all parts, laid end to end along the dimension named above; an argument that names none is the same for every part.
All inputs are finite; a program needn't handle non-finite values.
Results may differ from the reference program's by a relative error of at most 0.0149361.
Values are sent between devices in bfloat16 or wider.
A program may use at most 768 MiB of HBM per device.

```python
import jax
import jax.numpy as jnp
import numpy as np
from jax import lax

EP_SIZE = 8
TOK_DEV = 128
SEQ_LEN = 32
D_MODEL = 4096
D_FF = 960
Q_HEADS = 32
KV_HEADS = 8
HEAD_DIM = 128
EXPERTS = 16
TOKENS = EP_SIZE * TOK_DEV
CAP_SLOTS = 4 * TOK_DEV // EXPERTS
NORM_EPS = 1e-5
ROPE_THETA = 1000000.0


def route_pairs(rng_key):
    perm_key, tok_key, swap_key = jax.random.split(rng_key, 3)
    counts = np.array([4 * TOK_DEV // EXPERTS, TOK_DEV // EXPERTS, TOK_DEV // EXPERTS] + [2 * TOK_DEV // EXPERTS] * (EXPERTS - 3))
    rank_seq = jnp.asarray(np.repeat(np.arange(EXPERTS), counts), dtype=jnp.int32)
    expert_perm = jax.random.permutation(perm_key, EXPERTS).astype(jnp.int32)
    choice_seq = expert_perm[rank_seq]
    tok_perm = jax.random.permutation(tok_key, TOK_DEV)
    first_pick = choice_seq[:TOK_DEV][tok_perm]
    second_pick = choice_seq[TOK_DEV:][tok_perm]
    swap_bits = jax.random.randint(swap_key, (TOK_DEV,), 0, 2)
    lead_ids = jnp.where(swap_bits == 1, second_pick, first_pick)
    trail_ids = jnp.where(swap_bits == 1, first_pick, second_pick)
    return jnp.stack([lead_ids, trail_ids], axis=1)


def setup_inputs(seed: int = 0, part: int = 0) -> dict:
    root_key = jax.random.key(seed)
    part_keys = jax.random.split(jax.random.fold_in(root_key, part), 5)
    shared_keys = jax.random.split(jax.random.key(seed + 1), 10)
    q_dim = Q_HEADS * HEAD_DIM
    kv_dim = KV_HEADS * HEAD_DIM
    cache_shape = (TOKENS, SEQ_LEN, KV_HEADS, HEAD_DIM)
    hidden = jax.random.normal(part_keys[0], (TOKENS, D_MODEL), jnp.float32).astype(jnp.bfloat16)
    k_cache = (2.5 * jax.random.normal(part_keys[1], cache_shape, jnp.float32)).astype(jnp.bfloat16)
    v_cache = jax.random.normal(part_keys[2], cache_shape, jnp.float32).astype(jnp.bfloat16)
    seq_lens = jax.random.randint(part_keys[3], (TOKENS,), 0, SEQ_LEN).astype(jnp.int32).at[0].set(SEQ_LEN - 1)
    expert_ids = jax.vmap(route_pairs)(jax.random.split(part_keys[4], EP_SIZE)).reshape(TOKENS, 2)
    attn_gain = jax.random.uniform(shared_keys[0], (D_MODEL,), jnp.float32, 0.5, 1.5).astype(jnp.bfloat16)
    w_query = (jax.random.normal(shared_keys[1], (D_MODEL, q_dim), jnp.float32) * D_MODEL ** -0.5).astype(jnp.bfloat16)
    w_key = (jax.random.normal(shared_keys[2], (D_MODEL, kv_dim), jnp.float32) * D_MODEL ** -0.5).astype(jnp.bfloat16)
    w_value = (jax.random.normal(shared_keys[3], (D_MODEL, kv_dim), jnp.float32) * D_MODEL ** -0.5).astype(jnp.bfloat16)
    w_out = (jax.random.normal(shared_keys[4], (q_dim, D_MODEL), jnp.float32) * 2.0 * q_dim ** -0.5).astype(jnp.bfloat16)
    ffn_gain = jax.random.uniform(shared_keys[5], (D_MODEL,), jnp.float32, 0.5, 1.5).astype(jnp.bfloat16)
    w_router = (jax.random.normal(shared_keys[6], (D_MODEL, EXPERTS), jnp.float32) * D_MODEL ** -0.5).astype(jnp.bfloat16)
    w_gate = (jax.random.normal(shared_keys[7], (EXPERTS, D_MODEL, D_FF), jnp.float32) * D_MODEL ** -0.5).astype(jnp.bfloat16)
    w_up = (jax.random.normal(shared_keys[8], (EXPERTS, D_MODEL, D_FF), jnp.float32) * D_MODEL ** -0.5).astype(jnp.bfloat16)
    w_down = (jax.random.normal(shared_keys[9], (EXPERTS, D_FF, D_MODEL), jnp.float32) * 1.5 * D_FF ** -0.5).astype(jnp.bfloat16)
    return {'hidden': hidden, 'k_cache': k_cache, 'v_cache': v_cache, 'seq_lens': seq_lens, 'expert_ids': expert_ids, 'attn_gain': attn_gain, 'w_query': w_query, 'w_key': w_key, 'w_value': w_value, 'w_out': w_out, 'ffn_gain': ffn_gain, 'w_router': w_router, 'w_gate': w_gate, 'w_up': w_up, 'w_down': w_down}


def rms_scale(row_block, gain_vec):
    rows_f32 = row_block.astype(jnp.float32)
    inv_rms = lax.rsqrt(jnp.mean(rows_f32 * rows_f32, axis=-1, keepdims=True) + NORM_EPS)
    return (rows_f32 * inv_rms * gain_vec.astype(jnp.float32)).astype(jnp.bfloat16)


def rope_rotate(vectors, positions):
    half_dim = HEAD_DIM // 2
    inv_freq = ROPE_THETA ** (-2.0 * jnp.arange(half_dim, dtype=jnp.float32) / HEAD_DIM)
    angles = positions.astype(jnp.float32)[:, None, None] * inv_freq
    cosines = jnp.cos(angles)
    sine_vals = jnp.sin(angles)
    vec_f32 = vectors.astype(jnp.float32)
    low_half = vec_f32[..., :half_dim]
    high_half = vec_f32[..., half_dim:]
    return jnp.concatenate([low_half * cosines - high_half * sine_vals, high_half * cosines + low_half * sine_vals], axis=-1).astype(jnp.bfloat16)


def reference(hidden, k_cache, v_cache, seq_lens, expert_ids, attn_gain, w_query, w_key, w_value, w_out, ffn_gain, w_router, w_gate, w_up, w_down):
    groups = Q_HEADS // KV_HEADS
    normed = rms_scale(hidden, attn_gain)
    q_proj = jnp.dot(normed, w_query, preferred_element_type=jnp.float32).astype(jnp.bfloat16)
    q_proj = rope_rotate(q_proj.reshape(TOKENS, Q_HEADS, HEAD_DIM), seq_lens)
    key_new = jnp.dot(normed, w_key, preferred_element_type=jnp.float32).astype(jnp.bfloat16)
    key_new = rope_rotate(key_new.reshape(TOKENS, KV_HEADS, HEAD_DIM), seq_lens)
    value_new = jnp.dot(normed, w_value, preferred_element_type=jnp.float32).astype(jnp.bfloat16).reshape(TOKENS, KV_HEADS, HEAD_DIM)
    positions = jnp.arange(SEQ_LEN)
    slot_hit = (positions[None, :] == seq_lens[:, None])[:, :, None, None]
    k_cache_new = jnp.where(slot_hit, key_new[:, None], k_cache)
    v_cache_new = jnp.where(slot_hit, value_new[:, None], v_cache)

    def attend_one(operands):
        q_row, k_rows, v_rows, cur_len = operands
        q_grouped = q_row.reshape(KV_HEADS, groups, HEAD_DIM).astype(jnp.float32)
        scores = jnp.einsum('kgh,skh->kgs', q_grouped, k_rows.astype(jnp.float32)) * HEAD_DIM ** -0.5
        scores = jnp.where(positions[None, None, :] <= cur_len, scores, -jnp.inf)
        attn_probs = jax.nn.softmax(scores, axis=-1).astype(jnp.bfloat16)
        attn_mix = jnp.einsum('kgs,skh->kgh', attn_probs.astype(jnp.float32), v_rows.astype(jnp.float32))
        return attn_mix.astype(jnp.bfloat16).reshape(Q_HEADS * HEAD_DIM)

    attn_flat = lax.map(attend_one, (q_proj, k_cache_new, v_cache_new, seq_lens))
    resid_out = (hidden.astype(jnp.float32) + jnp.dot(attn_flat, w_out, preferred_element_type=jnp.float32)).astype(jnp.bfloat16)
    normed_ffn = rms_scale(resid_out, ffn_gain)
    logits = jnp.dot(normed_ffn, w_router, preferred_element_type=jnp.float32)
    gates = jax.nn.softmax(jnp.take_along_axis(logits, expert_ids, axis=1), axis=-1)
    flat_ids = expert_ids.reshape(-1)
    hit_table = (flat_ids[:, None] == jnp.arange(EXPERTS)[None, :]).astype(jnp.int32)
    slot_rank = jnp.sum((jnp.cumsum(hit_table, axis=0) - hit_table) * hit_table, axis=1)
    expert_cap = EP_SIZE * CAP_SLOTS
    flat_slot = flat_ids * expert_cap + slot_rank
    owner_tok = jnp.zeros((EXPERTS * expert_cap,), jnp.int32).at[flat_slot].set(jnp.arange(2 * TOKENS, dtype=jnp.int32) // 2)
    expert_rows = normed_ffn[owner_tok].reshape(EXPERTS, expert_cap, D_MODEL)

    def expert_ffn(operands):
        row_block, gate_mat, up_mat, down_mat = operands
        act_vals = jax.nn.silu(jnp.dot(row_block, gate_mat, preferred_element_type=jnp.float32)) * jnp.dot(row_block, up_mat, preferred_element_type=jnp.float32)
        return jnp.dot(act_vals.astype(jnp.bfloat16), down_mat, preferred_element_type=jnp.float32).astype(jnp.bfloat16)

    expert_out = lax.map(expert_ffn, (expert_rows, w_gate, w_up, w_down)).reshape(EXPERTS * expert_cap, D_MODEL)
    routed = expert_out[flat_slot].reshape(TOKENS, 2, D_MODEL).astype(jnp.float32)
    out_f32 = resid_out.astype(jnp.float32) + jnp.sum(gates[:, :, None] * routed, axis=1)
    return out_f32.astype(jnp.bfloat16), k_cache_new, v_cache_new
```

```python
import functools

import jax
import jax.numpy as jnp
import numpy as np
from jax import lax
from jax.experimental import pallas as pl
from jax.experimental.pallas import tpu as pltpu
from jax.sharding import PartitionSpec as P

NORM_EPS = 1e-5
ROPE_THETA = 1000000.0
VMEM_LIMIT = 67000000


def spread_gain(gain, gains):
    lanes = gain.shape[1]
    wide = gain[...].astype(jnp.float32)
    for r in range(gain.shape[0]):
        gains[:, r * lanes:(r + 1) * lanes] = wide[r:r + 1, :]


def column_of(row):
    return jnp.broadcast_to(row, (row.shape[1], row.shape[1])).T


def attn_kernel(
    lens, hidden, gain, lens_row, freq, wq, wk, wv, kc, vc,
    mix, kn, vn,
    normed, wbuf, kbuf, vbuf, heads, mixed, cos, sin, gains, wsem, ksem, vsem, kout, vout,
    *, kv_heads, tile, chunk,
):
    tokens, d_model = hidden.shape
    seq_len, head_dim = kc.shape[1], kc.shape[3]
    q_tiles, kv_tiles = wq.shape[1] // tile, wk.shape[1] // tile
    n_tiles = q_tiles + 2 * kv_tiles
    per_tile = tile // head_dim
    q_heads = wq.shape[1] // head_dim
    groups = q_heads // kv_heads
    pitch = tokens + 8
    slots = wbuf.shape[0]
    n_chunks = tokens // chunk

    def fetch(i, slot):
        @pl.when(i < q_tiles)
        def _():
            pltpu.make_async_copy(wq.at[:, pl.ds(pl.multiple_of(i * tile, tile), tile)], wbuf.at[slot], wsem.at[slot]).start()

        @pl.when(jnp.logical_and(i >= q_tiles, i < q_tiles + kv_tiles))
        def _():
            pltpu.make_async_copy(wk.at[:, pl.ds(pl.multiple_of((i - q_tiles) * tile, tile), tile)], wbuf.at[slot], wsem.at[slot]).start()

        @pl.when(jnp.logical_and(i >= q_tiles + kv_tiles, i < n_tiles))
        def _():
            pltpu.make_async_copy(wv.at[:, pl.ds(pl.multiple_of((i - q_tiles - kv_tiles) * tile, tile), tile)], wbuf.at[slot], wsem.at[slot]).start()

    def rows(c):
        return pl.ds(pl.multiple_of(c * chunk, chunk), chunk)

    for i in range(slots):
        fetch(jnp.int32(i), i)

    spread_gain(gain, gains)
    x = hidden[...].astype(jnp.float32)
    inv = lax.rsqrt(jnp.mean(x * x, axis=-1, keepdims=True) + NORM_EPS)
    normed[...] = (x * inv * gains[...]).astype(jnp.bfloat16)
    angles = column_of(lens_row[...].astype(jnp.float32)) * freq[...]
    sines = jnp.sin(angles)
    lane = lax.broadcasted_iota(jnp.int32, angles.shape, 1)
    cos[...] = jnp.cos(angles)
    sin[...] = jnp.where(lane < head_dim // 2, -sines, sines)

    def project(i, carry):
        slot = lax.rem(i, slots)
        pltpu.make_async_copy(wq.at[:, pl.ds(0, tile)], wbuf.at[slot], wsem.at[slot]).wait()
        out = jnp.dot(normed[...], wbuf[slot], preferred_element_type=jnp.float32)
        fetch(i + slots, slot)

        @pl.when(i + slots == n_tiles)
        def _():
            def start(c, carry):
                pltpu.make_async_copy(kc.at[rows(c)], kbuf.at[rows(c)], ksem.at[c]).start()
                pltpu.make_async_copy(vc.at[rows(c)], vbuf.at[rows(c)], vsem.at[c]).start()
                return carry

            lax.fori_loop(0, n_chunks, start, 0)

        turn = i < q_tiles + kv_tiles
        c_val = jnp.where(turn, cos[...], 1.0)
        s_val = jnp.where(turn, sin[...], 0.0)
        for j in range(per_tile):
            block = out[:, j * head_dim:(j + 1) * head_dim].astype(jnp.bfloat16).astype(jnp.float32)
            block = block * c_val + pltpu.roll(block, head_dim // 2, axis=1) * s_val
            block = block.astype(jnp.bfloat16).astype(jnp.float32)
            heads[pl.ds(pl.multiple_of((i * per_tile + j) * pitch, 8), tokens), :] = block
        return carry

    lax.fori_loop(0, n_tiles, project, 0)

    head_of = lax.broadcasted_iota(jnp.int32, (q_heads, seq_len * kv_heads), 0) // groups
    column = lax.broadcasted_iota(jnp.int32, (q_heads, seq_len * kv_heads), 1)
    own = head_of == lax.rem(column, kv_heads)

    def attend(c, carry):
        pltpu.make_async_copy(kc.at[rows(c)], kbuf.at[rows(c)], ksem.at[c]).wait()
        pltpu.make_async_copy(vc.at[rows(c)], vbuf.at[rows(c)], vsem.at[c]).wait()
        base = c * chunk
        for j in range(chunk):
            t = base + j
            n = lens[t]
            kbuf[t, n] = heads[pl.ds(q_heads * pitch + t, kv_heads, stride=pitch), :].astype(jnp.bfloat16)
            vbuf[t, n] = heads[pl.ds((q_heads + kv_heads) * pitch + t, kv_heads, stride=pitch), :].astype(jnp.bfloat16)
        probs = []
        for j in range(chunk):
            t = base + j
            q = heads[pl.ds(t, q_heads, stride=pitch), :].astype(jnp.bfloat16)
            keys = kbuf[t].reshape(seq_len * kv_heads, head_dim)
            score = lax.dot_general(q, keys, (((1,), (1,)), ((), ())), preferred_element_type=jnp.float32)
            score = score * head_dim ** -0.5
            seen = jnp.logical_and(own, column < (lens[t] + 1) * kv_heads)
            score = jnp.where(seen, score, -jnp.inf)
            e = jnp.exp(score - jnp.max(score, axis=-1, keepdims=True))
            probs.append((e / jnp.sum(e, axis=-1, keepdims=True)).astype(jnp.bfloat16))
        for j in range(chunk):
            t = base + j
            values = vbuf[t].reshape(seq_len * kv_heads, head_dim)
            o = jnp.dot(probs[j], values, preferred_element_type=jnp.float32)
            mixed[pl.ds(t, q_heads, stride=pitch), :] = o
        pltpu.make_async_copy(kbuf.at[rows(c)], kn.at[rows(c)], kout.at[c]).start()
        pltpu.make_async_copy(vbuf.at[rows(c)], vn.at[rows(c)], vout.at[c]).start()
        return carry

    lax.fori_loop(0, n_chunks, attend, 0)

    for h in range(q_heads):
        mix[:, h * head_dim:(h + 1) * head_dim] = mixed[h * pitch:h * pitch + tokens, :].astype(jnp.bfloat16)

    def drain(c, carry):
        pltpu.make_async_copy(kbuf.at[rows(c)], kn.at[rows(c)], kout.at[c]).wait()
        pltpu.make_async_copy(vbuf.at[rows(c)], vn.at[rows(c)], vout.at[c]).wait()
        return carry

    lax.fori_loop(0, n_chunks, drain, 0)


def attention(hidden, k_cache, v_cache, seq_lens, attn_gain, w_query, w_key, w_value):
    tokens, seq_len, kv_heads, head_dim = k_cache.shape
    d_model = hidden.shape[1]
    n_heads = w_query.shape[1] // head_dim
    all_heads = n_heads + 2 * kv_heads
    half = head_dim // 2
    inv_freq = np.float32(ROPE_THETA) ** (np.float32(-2.0) * np.arange(half, dtype=np.float32) / np.float32(head_dim))
    freq = jnp.asarray(np.concatenate([inv_freq, inv_freq])[None], jnp.float32)
    tile, chunk, slots = 512, 16, 3
    n_chunks = tokens // chunk
    vmem = pl.BlockSpec(memory_space=pltpu.VMEM)
    hbm = pl.BlockSpec(memory_space=pl.ANY)
    return pl.pallas_call(
        functools.partial(attn_kernel, kv_heads=kv_heads, tile=tile, chunk=chunk),
        out_shape=(
            jax.ShapeDtypeStruct((tokens, n_heads * head_dim), jnp.bfloat16),
            jax.ShapeDtypeStruct(k_cache.shape, jnp.bfloat16),
            jax.ShapeDtypeStruct(v_cache.shape, jnp.bfloat16),
        ),
        in_specs=[pl.BlockSpec(memory_space=pltpu.SMEM)] + [vmem] * 4 + [hbm] * 5,
        out_specs=(vmem, hbm, hbm),
        scratch_shapes=[
            pltpu.VMEM((tokens, d_model), jnp.bfloat16),
            pltpu.VMEM((slots, d_model, tile), jnp.bfloat16),
            pltpu.VMEM(k_cache.shape, jnp.bfloat16),
            pltpu.VMEM(v_cache.shape, jnp.bfloat16),
            pltpu.VMEM((all_heads * (tokens + 8), head_dim), jnp.float32),
            pltpu.VMEM((n_heads * (tokens + 8), head_dim), jnp.float32),
            pltpu.VMEM((tokens, head_dim), jnp.float32),
            pltpu.VMEM((tokens, head_dim), jnp.float32),
            pltpu.VMEM((1, d_model), jnp.float32),
            pltpu.SemaphoreType.DMA((slots,)),
            pltpu.SemaphoreType.DMA((n_chunks,)),
            pltpu.SemaphoreType.DMA((n_chunks,)),
            pltpu.SemaphoreType.DMA((n_chunks,)),
            pltpu.SemaphoreType.DMA((n_chunks,)),
        ],
        compiler_params=pltpu.CompilerParams(vmem_limit_bytes=VMEM_LIMIT),
        name="attend",
    )(seq_lens, hidden, attn_gain.reshape(-1, 128), seq_lens.reshape(1, tokens), freq, w_query, w_key, w_value, k_cache, v_cache)


MESH_ID = pl.DeviceIdType.MESH


def moe_kernel(
    mix, hidden, ids_row, gain, router, wo, wg, wu, wd,
    out,
    gbuf, wdbuf, xall, rows_buf, inner, ret, sel_out, sel_in, comb, gates, gains,
    wo_sem, wg_sem, wd_sem, xsend, xrecv, sel_send, sel_recv, ysend, yrecv,
    *, n_ep, tile, cap,
):
    tokens, d_model = hidden.shape
    d_ff = wg.shape[1]
    local = wg.shape[0]
    n_experts = local * n_ep
    tiles = d_model // tile
    ring = n_ep // 2
    slab = local * cap
    near = 6 * cap
    f32, bf16 = jnp.float32, jnp.bfloat16
    last = (((1,), (1,)), ((), ()))

    me = lax.axis_index('ep')
    x, c = me // 2, lax.rem(me, 2)

    def at(step, core):
        return lax.rem(x + step, ring) * 2 + core

    other = 1 - c
    peers = [me, at(0, other), at(ring - 1, c), at(ring - 1, other), at(1, c), at(1, other), at(2, c), at(2, other)]
    partner, left, left2, right, right2, far, far2 = peers[1:]

    def cols(i):
        return pl.ds(pl.multiple_of(i * tile, tile), tile)

    parts = d_model // tile

    def wo_start(i, slot):
        for j in range(parts):
            span = slice(j * tile, (j + 1) * tile)
            pltpu.make_async_copy(wo.at[span, cols(i)], gbuf.at[slot, 0:tile, span], wo_sem.at[slot]).start()

    def wo_wait(slot):
        pltpu.make_async_copy(wo.at[0:tile, :], gbuf.at[slot, 0:tile, :], wo_sem.at[slot]).wait()

    def ff_copy(g):
        src = wg if g % 2 == 0 else wu
        return pltpu.make_async_copy(src.at[g // 2], gbuf.at[g], wg_sem.at[g])

    wd_slots = wdbuf.shape[0]
    wd_total = 2 * local * tiles

    def wd_copy(q):
        e = lax.rem(q // tiles, local)
        slot = lax.rem(q, wd_slots)
        return pltpu.make_async_copy(wd.at[e, :, cols(lax.rem(q, tiles))], wdbuf.at[slot], wd_sem.at[slot])

    for i in range(4):
        wo_start(i, i)

    barrier = pltpu.get_barrier_semaphore()
    for peer in peers[1:]:
        pl.semaphore_signal(barrier, inc=1, device_id={'ep': peer}, device_id_type=MESH_ID)
    pl.semaphore_wait(barrier, n_ep - 1)

    t_sub = lax.broadcasted_iota(jnp.int32, (tokens, tokens), 0)
    t_lane = lax.broadcasted_iota(jnp.int32, (tokens, tokens), 1)
    id0_row, id1_row = ids_row[0:1, :].astype(f32), ids_row[1:2, :].astype(f32)
    e_sub = lax.broadcasted_iota(jnp.int32, (n_experts, tokens), 0).astype(f32)
    spread_gain(gain, gains)
    hit_row = jnp.logical_or(e_sub == id0_row, e_sub == id1_row).astype(f32).astype(bf16)
    rank_row = jnp.dot(hit_row, (t_sub < t_lane).astype(f32).astype(bf16), preferred_element_type=f32)
    slots_row = []
    for ident in (id0_row, id1_row):
        rank = jnp.sum(jnp.where(e_sub == ident, rank_row, 0.0), axis=0, keepdims=True)
        slots_row.append(ident * cap + rank)
    for d in range(n_ep):
        want = (lax.broadcasted_iota(jnp.int32, (slab, tokens), 0) + d * slab).astype(f32)
        pick = jnp.logical_or(want == slots_row[0], want == slots_row[1])
        sel_out[d] = pick.astype(f32).astype(bf16)
    for k in range(1, n_ep):
        pltpu.make_async_remote_copy(
            src_ref=sel_out.at[peers[k]], dst_ref=sel_in.at[me], send_sem=sel_send, recv_sem=sel_recv,
            device_id={'ep': peers[k]}, device_id_type=MESH_ID,
        ).start()
    sel_in[me] = sel_out[me]

    id0, id1 = column_of(id0_row)[:, 0:1], column_of(id1_row)[:, 0:1]
    e_lane = lax.broadcasted_iota(jnp.int32, (tokens, n_experts), 1).astype(f32)
    hit = jnp.logical_or(e_lane == id0, e_lane == id1).astype(f32).astype(bf16)
    rank_col = jnp.dot((t_lane < t_sub).astype(f32).astype(bf16), hit, preferred_element_type=f32)
    s_lane = lax.broadcasted_iota(jnp.int32, (tokens, n_experts * cap), 1).astype(f32)
    for k, ident in enumerate((id0, id1)):
        rank = jnp.sum(jnp.where(e_lane == ident, rank_col, 0.0), axis=1, keepdims=True)
        comb[k * tokens:(k + 1) * tokens, :] = (s_lane == ident * cap + rank).astype(f32).astype(bf16)

    def x_copy(src, i, dev, kind):
        return pltpu.make_async_remote_copy(
            src_ref=xall.at[src, i], dst_ref=xall.at[src, i], send_sem=xsend.at[kind, i], recv_sem=xrecv.at[src, i],
            device_id={'ep': dev}, device_id_type=MESH_ID,
        )

    def arrived(src, i):
        pltpu.make_async_copy(xall.at[src, i], xall.at[src, i], xrecv.at[src, i]).wait()

    def project(i, carry):
        slot = lax.rem(i, 4)
        wo_wait(slot)
        acc = jnp.zeros((tokens, tile), f32)
        for j in range(parts):
            span = slice(j * tile, (j + 1) * tile)
            acc = acc + jnp.dot(mix[:, span], gbuf[slot, 0:tile, span], preferred_element_type=f32)
        xall[me, i] = (hidden[:, cols(i)].astype(f32) + acc).astype(bf16)
        x_copy(me, i, right, 0).start()
        x_copy(me, i, left, 1).start()
        x_copy(me, i, partner, 2).start()

        @pl.when(i < 4)
        def _():
            wo_start(i + 4, slot)

        for g in range(4):
            @pl.when(i == g + 4)
            def _():
                ff_copy(g).start()
        return carry

    lax.fori_loop(0, tiles, project, 0)
    for q in range(wd_slots):
        wd_copy(jnp.int32(q)).start()

    def square(i, acc):
        v = xall[me, i].astype(f32)
        return acc + jnp.sum(v * v, axis=1, keepdims=True)

    inv = lax.rsqrt(lax.fori_loop(0, tiles, square, jnp.zeros((tokens, 1), f32)) / d_model + NORM_EPS)

    def route(i, acc):
        v = (xall[me, i].astype(f32) * inv * gains[:, cols(i)]).astype(bf16)
        return acc + lax.dot_general(v, router[:, cols(i)], last, preferred_element_type=f32)

    logits = lax.fori_loop(0, tiles, route, jnp.zeros((tokens, n_experts), f32))
    l0 = jnp.sum(jnp.where(e_lane == id0, logits, 0.0), axis=1, keepdims=True)
    l1 = jnp.sum(jnp.where(e_lane == id1, logits, 0.0), axis=1, keepdims=True)
    top = jnp.maximum(l0, l1)
    e0, e1 = jnp.exp(l0 - top), jnp.exp(l1 - top)
    gates[0] = jnp.broadcast_to(e0 / (e0 + e1), (tokens, 128))
    gates[1] = jnp.broadcast_to(e1 / (e0 + e1), (tokens, 128))

    def gather(src, pos, i):
        got = jnp.dot(sel_in[src], xall[src, i], preferred_element_type=f32).astype(bf16)
        for e in range(local):
            rows_buf[e, pos * cap:(pos + 1) * cap, cols(i)] = got[e * cap:(e + 1) * cap]

    pltpu.make_async_copy(sel_in.at[pl.ds(0, n_ep - 1)], sel_in.at[pl.ds(0, n_ep - 1)], sel_recv).wait()

    def own(i, carry):
        gather(me, 0, i)
        return carry

    lax.fori_loop(0, tiles, own, 0)

    def neighbours(i, carry):
        arrived(left, i)
        x_copy(left, i, partner, 4).start()

        @pl.when(lax.rem(i, 2) == 0)
        def _():
            x_copy(left, i, right, 3).start()

        gather(left, 2, i)
        arrived(right, i)
        x_copy(right, i, partner, 5).start()

        @pl.when(lax.rem(i, 2) == 1)
        def _():
            x_copy(right, i, left, 3).start()

        gather(right, 4, i)
        arrived(partner, i)
        gather(partner, 1, i)
        return carry

    lax.fori_loop(0, tiles, neighbours, 0)

    def neighbours2(i, carry):
        arrived(left2, i)
        gather(left2, 3, i)
        arrived(right2, i)
        gather(right2, 5, i)
        return carry

    lax.fori_loop(0, tiles, neighbours2, 0)

    def across(i, carry):
        arrived(far, i)
        x_copy(far, i, partner, 6).start()
        gather(far, 6, i)
        return carry

    def across2(i, carry):
        arrived(far2, i)
        gather(far2, 7, i)
        return carry

    block = 16

    def normalise(first, count):
        def step(r, carry):
            rows = pl.ds(pl.multiple_of(first + r * block, block), block)
            for e in range(local):
                acc = jnp.zeros((block, tile), f32)
                for i in range(tiles):
                    v = rows_buf[e, rows, i * tile:(i + 1) * tile].astype(f32)
                    acc = acc + v * v
                scale = lax.rsqrt(jnp.sum(acc, axis=1, keepdims=True) / d_model + NORM_EPS)
                for i in range(tiles):
                    span = slice(i * tile, (i + 1) * tile)
                    v = rows_buf[e, rows, span].astype(f32)
                    rows_buf[e, rows, span] = (v * scale * gains[:, span]).astype(bf16)
            return carry

        lax.fori_loop(0, count // block, step, 0)

    def expand(e, first, count, fetched):
        for g in (2 * e, 2 * e + 1):
            if not fetched:
                ff_copy(g).wait()
        for lo in range(0, d_ff, 512):
            hi = min(lo + 512, d_ff)
            up_in = rows_buf[e, first:first + count, :]
            gate = lax.dot_general(up_in, gbuf[2 * e, lo:hi, :], last, preferred_element_type=f32)
            up = lax.dot_general(up_in, gbuf[2 * e + 1, lo:hi, :], last, preferred_element_type=f32)
            inner[first:first + count, lo:hi] = (jax.nn.silu(gate) * up).astype(bf16)

    def y_copy(e, i, pos):
        return pltpu.make_async_remote_copy(
            src_ref=rows_buf.at[e, pl.ds(pos * cap, cap), cols(i)],
            dst_ref=ret.at[pl.ds(pl.multiple_of((me * local + e) * cap, cap), cap), cols(i)],
            send_sem=ysend.at[e, i], recv_sem=yrecv.at[e, i],
            device_id={'ep': peers[pos]}, device_id_type=MESH_ID,
        )

    def contract(e, first, count, base):
        def step(i, carry):
            q = base + i
            wd_copy(q).wait()
            y = jnp.dot(inner[first:first + count, :], wdbuf[lax.rem(q, wd_slots)], preferred_element_type=f32).astype(bf16)

            @pl.when(q + wd_slots < wd_total)
            def _():
                wd_copy(q + wd_slots).start()

            rows_buf[e, first:first + count, cols(i)] = y
            if first == 0:
                ret[pl.ds(pl.multiple_of((me * local + e) * cap, cap), cap), cols(i)] = y[:cap]
            for pos in range(max(first // cap, 1), (first + count) // cap):
                y_copy(e, i, pos).start()
            return carry

        lax.fori_loop(0, tiles, step, 0)

    rest = n_ep * cap - near
    normalise(0, near)
    expand(0, 0, near, False)
    lax.fori_loop(0, tiles // 2, across, 0)
    contract(0, 0, near, 0)
    expand(1, 0, near, False)
    lax.fori_loop(tiles // 2, tiles, across, 0)
    contract(1, 0, near, tiles)
    lax.fori_loop(0, tiles, across2, 0)
    normalise(near, rest)
    expand(0, near, rest, True)
    contract(0, near, rest, 2 * tiles)
    expand(1, near, rest, True)
    contract(1, near, rest, 3 * tiles)

    whole = pl.ds(0, (n_ep - 1) * cap)

    def finish(i, carry):
        for e in range(local):
            pltpu.make_async_copy(ret.at[whole, cols(i)], ret.at[whole, cols(i)], yrecv.at[e, i]).wait()
        picked = jnp.dot(comb[...], ret[:, cols(i)], preferred_element_type=f32)
        reps = tile // 128
        g0 = jnp.concatenate([gates[0]] * reps, axis=1)
        g1 = jnp.concatenate([gates[1]] * reps, axis=1)
        out[:, cols(i)] = (xall[me, i].astype(f32) + (g0 * picked[:tokens] + g1 * picked[tokens:])).astype(bf16)
        return carry

    lax.fori_loop(0, tiles, finish, 0)

    def drain(i, carry):
        for kind in (0, 1, 2, 3, 4, 5, 6):
            pltpu.make_async_copy(xall.at[0, i], xall.at[0, i], xsend.at[kind, i]).wait()
        for e in range(local):
            pltpu.make_async_copy(ret.at[whole, cols(i)], ret.at[whole, cols(i)], ysend.at[e, i]).wait()
        return carry

    lax.fori_loop(0, tiles, drain, 0)
    pltpu.make_async_copy(sel_in.at[pl.ds(0, n_ep - 1)], sel_in.at[pl.ds(0, n_ep - 1)], sel_send).wait()


def moe(mix, hidden, expert_ids, ffn_gain, w_out, w_router, w_gate, w_up, w_down, n_ep):
    tokens, d_model = hidden.shape
    local, _, d_ff = w_gate.shape
    n_experts = local * n_ep
    cap = 4 * tokens // n_experts
    tile = 512
    tiles = d_model // tile
    vmem = pl.BlockSpec(memory_space=pltpu.VMEM)
    hbm = pl.BlockSpec(memory_space=pl.ANY)
    dma = pltpu.SemaphoreType.DMA
    return pl.pallas_call(
        functools.partial(moe_kernel, n_ep=n_ep, tile=tile, cap=cap),
        out_shape=jax.ShapeDtypeStruct((tokens, d_model), jnp.bfloat16),
        in_specs=[vmem] * 5 + [hbm] * 4,
        out_specs=vmem,
        scratch_shapes=[
            pltpu.VMEM((2 * local, d_ff, d_model), jnp.bfloat16),
            pltpu.VMEM((4, d_ff, tile), jnp.bfloat16),
            pltpu.VMEM((n_ep, tiles, tokens, tile), jnp.bfloat16),
            pltpu.VMEM((local, n_ep * cap, d_model), jnp.bfloat16),
            pltpu.VMEM((n_ep * cap, d_ff), jnp.bfloat16),
            pltpu.VMEM((n_experts * cap, d_model), jnp.bfloat16),
            pltpu.VMEM((n_ep, local * cap, tokens), jnp.bfloat16),
            pltpu.VMEM((n_ep, local * cap, tokens), jnp.bfloat16),
            pltpu.VMEM((2 * tokens, n_experts * cap), jnp.bfloat16),
            pltpu.VMEM((2, tokens, 128), jnp.float32),
            pltpu.VMEM((1, d_model), jnp.float32),
            dma((4,)), dma((4,)), dma((4,)),
            dma((7, tiles)), dma((n_ep, tiles)),
            dma, dma,
            dma((local, tiles)), dma((local, tiles)),
        ],
        compiler_params=pltpu.CompilerParams(collective_id=0, has_side_effects=True, vmem_limit_bytes=VMEM_LIMIT),
        name="moe",
    )(mix, hidden, expert_ids.T, ffn_gain.reshape(-1, 128), w_router.T, w_out, w_gate.transpose(0, 2, 1), w_up.transpose(0, 2, 1), w_down)


def solution(mesh):
    n_ep = mesh.shape['ep']
    row_spec = P(('dp', 'ep'), None)
    cache_spec = P(('dp', 'ep'), None, None, None)
    expert_spec = P('ep', None, None)
    in_specs = (row_spec, cache_spec, cache_spec, P(('dp', 'ep')), row_spec, P(), P(), P(), P(), P(), P(), P(), expert_spec, expert_spec, expert_spec)
    out_specs = (row_spec, cache_spec, cache_spec)

    def device_step(hidden, k_cache, v_cache, seq_lens, expert_ids, attn_gain, w_query, w_key, w_value, w_out, ffn_gain, w_router, w_gate, w_up, w_down):
        mix, k_cache_new, v_cache_new = attention(hidden, k_cache, v_cache, seq_lens, attn_gain, w_query, w_key, w_value)
        out = moe(mix, hidden, expert_ids, ffn_gain, w_out, w_router, w_gate, w_up, w_down, n_ep)
        return out, k_cache_new, v_cache_new

    return jax.shard_map(device_step, mesh=mesh, in_specs=in_specs, out_specs=out_specs, check_vma=False)
```

```python
import functools

import jax
import jax.numpy as jnp
import numpy as np
from jax import lax
from jax.experimental import pallas as pl
from jax.experimental.pallas import tpu as pltpu
from jax.sharding import PartitionSpec as P

NORM_EPS = 1e-5
ROPE_THETA = 1000000.0
VMEM_LIMIT = 67000000


def spread_gain(gain, gains):
    lanes = gain.shape[1]
    wide = gain[...].astype(jnp.float32)
    for r in range(gain.shape[0]):
        gains[:, r * lanes:(r + 1) * lanes] = wide[r:r + 1, :]


def column_of(row):
    return jnp.broadcast_to(row, (row.shape[1], row.shape[1])).T


def attn_kernel(
    lens, hidden, gain, lens_row, freq, wq, wk, wv, kc, vc,
    mix, kn, vn,
    normed, wbuf, kbuf, vbuf, heads, mixed, cos, sin, gains, wsem, ksem, vsem, kout, vout,
    *, kv_heads, tile, chunk,
):
    tokens, d_model = hidden.shape
    seq_len, head_dim = kc.shape[1], kc.shape[3]
    q_tiles, kv_tiles = wq.shape[1] // tile, wk.shape[1] // tile
    n_tiles = q_tiles + 2 * kv_tiles
    per_tile = tile // head_dim
    q_heads = wq.shape[1] // head_dim
    groups = q_heads // kv_heads
    pitch = tokens + 8
    slots = wbuf.shape[0]
    n_chunks = tokens // chunk

    def fetch(i, slot):
        @pl.when(i < q_tiles)
        def _():
            pltpu.make_async_copy(wq.at[:, pl.ds(pl.multiple_of(i * tile, tile), tile)], wbuf.at[slot], wsem.at[slot]).start()

        @pl.when(jnp.logical_and(i >= q_tiles, i < q_tiles + kv_tiles))
        def _():
            pltpu.make_async_copy(wk.at[:, pl.ds(pl.multiple_of((i - q_tiles) * tile, tile), tile)], wbuf.at[slot], wsem.at[slot]).start()

        @pl.when(jnp.logical_and(i >= q_tiles + kv_tiles, i < n_tiles))
        def _():
            pltpu.make_async_copy(wv.at[:, pl.ds(pl.multiple_of((i - q_tiles - kv_tiles) * tile, tile), tile)], wbuf.at[slot], wsem.at[slot]).start()

    def rows(c):
        return pl.ds(pl.multiple_of(c * chunk, chunk), chunk)

    for i in range(slots):
        fetch(jnp.int32(i), i)

    spread_gain(gain, gains)
    x = hidden[...].astype(jnp.float32)
    inv = lax.rsqrt(jnp.mean(x * x, axis=-1, keepdims=True) + NORM_EPS)
    normed[...] = (x * inv * gains[...]).astype(jnp.bfloat16)
    angles = column_of(lens_row[...].astype(jnp.float32)) * freq[...]
    sines = jnp.sin(angles)
    lane = lax.broadcasted_iota(jnp.int32, angles.shape, 1)
    cos[...] = jnp.cos(angles)
    sin[...] = jnp.where(lane < head_dim // 2, -sines, sines)

    def project(i, carry):
        slot = lax.rem(i, slots)
        pltpu.make_async_copy(wq.at[:, pl.ds(0, tile)], wbuf.at[slot], wsem.at[slot]).wait()
        out = jnp.dot(normed[...], wbuf[slot], preferred_element_type=jnp.float32)
        fetch(i + slots, slot)

        @pl.when(i + slots == n_tiles)
        def _():
            def start(c, carry):
                pltpu.make_async_copy(kc.at[rows(c)], kbuf.at[rows(c)], ksem.at[c]).start()
                pltpu.make_async_copy(vc.at[rows(c)], vbuf.at[rows(c)], vsem.at[c]).start()
                return carry

            lax.fori_loop(0, n_chunks, start, 0)

        turn = i < q_tiles + kv_tiles
        c_val = jnp.where(turn, cos[...], 1.0)
        s_val = jnp.where(turn, sin[...], 0.0)
        for j in range(per_tile):
            block = out[:, j * head_dim:(j + 1) * head_dim].astype(jnp.bfloat16).astype(jnp.float32)
            block = block * c_val + pltpu.roll(block, head_dim // 2, axis=1) * s_val
            block = block.astype(jnp.bfloat16).astype(jnp.float32)
            heads[pl.ds(pl.multiple_of((i * per_tile + j) * pitch, 8), tokens), :] = block
        return carry

    lax.fori_loop(0, n_tiles, project, 0)

    head_of = lax.broadcasted_iota(jnp.int32, (q_heads, seq_len * kv_heads), 0) // groups
    column = lax.broadcasted_iota(jnp.int32, (q_heads, seq_len * kv_heads), 1)
    own = head_of == lax.rem(column, kv_heads)

    def attend(c, carry):
        pltpu.make_async_copy(kc.at[rows(c)], kbuf.at[rows(c)], ksem.at[c]).wait()
        pltpu.make_async_copy(vc.at[rows(c)], vbuf.at[rows(c)], vsem.at[c]).wait()
        base = c * chunk
        for j in range(chunk):
            t = base + j
            n = lens[t]
            kbuf[t, n] = heads[pl.ds(q_heads * pitch + t, kv_heads, stride=pitch), :].astype(jnp.bfloat16)
            vbuf[t, n] = heads[pl.ds((q_heads + kv_heads) * pitch + t, kv_heads, stride=pitch), :].astype(jnp.bfloat16)
        probs = []
        for j in range(chunk):
            t = base + j
            q = heads[pl.ds(t, q_heads, stride=pitch), :].astype(jnp.bfloat16)
            keys = kbuf[t].reshape(seq_len * kv_heads, head_dim)
            score = lax.dot_general(q, keys, (((1,), (1,)), ((), ())), preferred_element_type=jnp.float32)
            score = score * head_dim ** -0.5
            seen = jnp.logical_and(own, column < (lens[t] + 1) * kv_heads)
            score = jnp.where(seen, score, -jnp.inf)
            e = jnp.exp(score - jnp.max(score, axis=-1, keepdims=True))
            probs.append((e / jnp.sum(e, axis=-1, keepdims=True)).astype(jnp.bfloat16))
        for j in range(chunk):
            t = base + j
            values = vbuf[t].reshape(seq_len * kv_heads, head_dim)
            o = jnp.dot(probs[j], values, preferred_element_type=jnp.float32)
            mixed[pl.ds(t, q_heads, stride=pitch), :] = o
        pltpu.make_async_copy(kbuf.at[rows(c)], kn.at[rows(c)], kout.at[c]).start()
        pltpu.make_async_copy(vbuf.at[rows(c)], vn.at[rows(c)], vout.at[c]).start()
        return carry

    lax.fori_loop(0, n_chunks, attend, 0)

    for h in range(q_heads):
        mix[:, h * head_dim:(h + 1) * head_dim] = mixed[h * pitch:h * pitch + tokens, :].astype(jnp.bfloat16)

    def drain(c, carry):
        pltpu.make_async_copy(kbuf.at[rows(c)], kn.at[rows(c)], kout.at[c]).wait()
        pltpu.make_async_copy(vbuf.at[rows(c)], vn.at[rows(c)], vout.at[c]).wait()
        return carry

    lax.fori_loop(0, n_chunks, drain, 0)


def attention(hidden, k_cache, v_cache, seq_lens, attn_gain, w_query, w_key, w_value):
    tokens, seq_len, kv_heads, head_dim = k_cache.shape
    d_model = hidden.shape[1]
    n_heads = w_query.shape[1] // head_dim
    all_heads = n_heads + 2 * kv_heads
    half = head_dim // 2
    inv_freq = np.float32(ROPE_THETA) ** (np.float32(-2.0) * np.arange(half, dtype=np.float32) / np.float32(head_dim))
    freq = jnp.asarray(np.concatenate([inv_freq, inv_freq])[None], jnp.float32)
    tile, chunk, slots = 512, 16, 3
    n_chunks = tokens // chunk
    vmem = pl.BlockSpec(memory_space=pltpu.VMEM)
    hbm = pl.BlockSpec(memory_space=pl.ANY)
    return pl.pallas_call(
        functools.partial(attn_kernel, kv_heads=kv_heads, tile=tile, chunk=chunk),
        out_shape=(
            jax.ShapeDtypeStruct((tokens, n_heads * head_dim), jnp.bfloat16),
            jax.ShapeDtypeStruct(k_cache.shape, jnp.bfloat16),
            jax.ShapeDtypeStruct(v_cache.shape, jnp.bfloat16),
        ),
        in_specs=[pl.BlockSpec(memory_space=pltpu.SMEM)] + [vmem] * 4 + [hbm] * 5,
        out_specs=(vmem, hbm, hbm),
        scratch_shapes=[
            pltpu.VMEM((tokens, d_model), jnp.bfloat16),
            pltpu.VMEM((slots, d_model, tile), jnp.bfloat16),
            pltpu.VMEM(k_cache.shape, jnp.bfloat16),
            pltpu.VMEM(v_cache.shape, jnp.bfloat16),
            pltpu.VMEM((all_heads * (tokens + 8), head_dim), jnp.float32),
            pltpu.VMEM((n_heads * (tokens + 8), head_dim), jnp.float32),
            pltpu.VMEM((tokens, head_dim), jnp.float32),
            pltpu.VMEM((tokens, head_dim), jnp.float32),
            pltpu.VMEM((1, d_model), jnp.float32),
            pltpu.SemaphoreType.DMA((slots,)),
            pltpu.SemaphoreType.DMA((n_chunks,)),
            pltpu.SemaphoreType.DMA((n_chunks,)),
            pltpu.SemaphoreType.DMA((n_chunks,)),
            pltpu.SemaphoreType.DMA((n_chunks,)),
        ],
        compiler_params=pltpu.CompilerParams(vmem_limit_bytes=VMEM_LIMIT),
        name="attend",
    )(seq_lens, hidden, attn_gain.reshape(-1, 128), seq_lens.reshape(1, tokens), freq, w_query, w_key, w_value, k_cache, v_cache)


MESH_ID = pl.DeviceIdType.MESH


def moe_kernel(
    mix, hidden, ids_row, gain, router, wo, wg, wu, wd,
    out,
    gbuf, wdbuf, xall, rows_buf, inner, ret, sel_out, sel_in, comb, gates, gains,
    wo_sem, wg_sem, wd_sem, xsend, xrecv, sel_send, sel_recv, ysend, yrecv,
    *, n_ep, tile, cap,
):
    tokens, d_model = hidden.shape
    d_ff = wg.shape[1]
    local = wg.shape[0]
    n_experts = local * n_ep
    tiles = d_model // tile
    ring = n_ep // 2
    slab = local * cap
    f32, bf16 = jnp.float32, jnp.bfloat16
    last = (((1,), (1,)), ((), ()))

    me = lax.axis_index('ep')
    x, c = me // 2, lax.rem(me, 2)

    def at(step, core):
        return lax.rem(x + step, ring) * 2 + core

    other = 1 - c
    peers = [me, at(0, other), at(ring - 1, c), at(ring - 1, other), at(1, c), at(1, other), at(2, c), at(2, other)]
    partner, left, left2, right, right2, far, far2 = peers[1:]

    def cols(i):
        return pl.ds(pl.multiple_of(i * tile, tile), tile)

    parts = d_model // tile

    def wo_start(i, slot):
        for j in range(parts):
            span = slice(j * tile, (j + 1) * tile)
            pltpu.make_async_copy(wo.at[span, cols(i)], gbuf.at[slot, 0:tile, span], wo_sem.at[slot]).start()

    def wo_wait(slot):
        pltpu.make_async_copy(wo.at[0:tile, :], gbuf.at[slot, 0:tile, :], wo_sem.at[slot]).wait()

    def ff_copy(g):
        src = wg if g % 2 == 0 else wu
        return pltpu.make_async_copy(src.at[g // 2], gbuf.at[g], wg_sem.at[g])

    wd_slots = wdbuf.shape[0]
    wd_total = local * tiles

    def wd_copy(q):
        e = lax.rem(q // tiles, local)
        slot = lax.rem(q, wd_slots)
        return pltpu.make_async_copy(wd.at[e, :, cols(lax.rem(q, tiles))], wdbuf.at[slot], wd_sem.at[slot])

    for i in range(4):
        wo_start(i, i)

    barrier = pltpu.get_barrier_semaphore()
    for peer in peers[1:]:
        pl.semaphore_signal(barrier, inc=1, device_id={'ep': peer}, device_id_type=MESH_ID)
    pl.semaphore_wait(barrier, n_ep - 1)

    t_sub = lax.broadcasted_iota(jnp.int32, (tokens, tokens), 0)
    t_lane = lax.broadcasted_iota(jnp.int32, (tokens, tokens), 1)
    id0_row, id1_row = ids_row[0:1, :].astype(f32), ids_row[1:2, :].astype(f32)
    e_sub = lax.broadcasted_iota(jnp.int32, (n_experts, tokens), 0).astype(f32)
    spread_gain(gain, gains)
    hit_row = jnp.logical_or(e_sub == id0_row, e_sub == id1_row).astype(f32).astype(bf16)
    rank_row = jnp.dot(hit_row, (t_sub < t_lane).astype(f32).astype(bf16), preferred_element_type=f32)
    slots_row = []
    for ident in (id0_row, id1_row):
        rank = jnp.sum(jnp.where(e_sub == ident, rank_row, 0.0), axis=0, keepdims=True)
        slots_row.append(ident * cap + rank)
    for d in range(n_ep):
        want = (lax.broadcasted_iota(jnp.int32, (slab, tokens), 0) + d * slab).astype(f32)
        pick = jnp.logical_or(want == slots_row[0], want == slots_row[1])
        sel_out[d] = pick.astype(f32).astype(bf16)
    for k in range(1, n_ep):
        pltpu.make_async_remote_copy(
            src_ref=sel_out.at[peers[k]], dst_ref=sel_in.at[me], send_sem=sel_send, recv_sem=sel_recv,
            device_id={'ep': peers[k]}, device_id_type=MESH_ID,
        ).start()
    sel_in[me] = sel_out[me]

    id0, id1 = column_of(id0_row)[:, 0:1], column_of(id1_row)[:, 0:1]
    e_lane = lax.broadcasted_iota(jnp.int32, (tokens, n_experts), 1).astype(f32)
    hit = jnp.logical_or(e_lane == id0, e_lane == id1).astype(f32).astype(bf16)
    rank_col = jnp.dot((t_lane < t_sub).astype(f32).astype(bf16), hit, preferred_element_type=f32)
    s_lane = lax.broadcasted_iota(jnp.int32, (tokens, n_experts * cap), 1).astype(f32)
    for k, ident in enumerate((id0, id1)):
        rank = jnp.sum(jnp.where(e_lane == ident, rank_col, 0.0), axis=1, keepdims=True)
        comb[k * tokens:(k + 1) * tokens, :] = (s_lane == ident * cap + rank).astype(f32).astype(bf16)

    def x_copy(src, i, dev, kind):
        return pltpu.make_async_remote_copy(
            src_ref=xall.at[src, i], dst_ref=xall.at[src, i], send_sem=xsend.at[kind, i], recv_sem=xrecv.at[src, i],
            device_id={'ep': dev}, device_id_type=MESH_ID,
        )

    def arrived(src, i):
        pltpu.make_async_copy(xall.at[src, i], xall.at[src, i], xrecv.at[src, i]).wait()

    def project(i, carry):
        slot = lax.rem(i, 4)
        wo_wait(slot)
        acc = jnp.zeros((tokens, tile), f32)
        for j in range(parts):
            span = slice(j * tile, (j + 1) * tile)
            acc = acc + jnp.dot(mix[:, span], gbuf[slot, 0:tile, span], preferred_element_type=f32)
        xall[me, i] = (hidden[:, cols(i)].astype(f32) + acc).astype(bf16)
        x_copy(me, i, right, 0).start()
        x_copy(me, i, left, 1).start()
        x_copy(me, i, partner, 2).start()

        @pl.when(i < 4)
        def _():
            wo_start(i + 4, slot)

        for g in range(4):
            @pl.when(i == g + 4)
            def _():
                ff_copy(g).start()
        return carry

    lax.fori_loop(0, tiles, project, 0)
    for q in range(wd_slots):
        wd_copy(jnp.int32(q)).start()

    def square(i, acc):
        v = xall[me, i].astype(f32)
        return acc + jnp.sum(v * v, axis=1, keepdims=True)

    inv = lax.rsqrt(lax.fori_loop(0, tiles, square, jnp.zeros((tokens, 1), f32)) / d_model + NORM_EPS)

    def route(i, acc):
        v = (xall[me, i].astype(f32) * inv * gains[:, cols(i)]).astype(bf16)
        return acc + lax.dot_general(v, router[:, cols(i)], last, preferred_element_type=f32)

    logits = lax.fori_loop(0, tiles, route, jnp.zeros((tokens, n_experts), f32))
    l0 = jnp.sum(jnp.where(e_lane == id0, logits, 0.0), axis=1, keepdims=True)
    l1 = jnp.sum(jnp.where(e_lane == id1, logits, 0.0), axis=1, keepdims=True)
    top = jnp.maximum(l0, l1)
    e0, e1 = jnp.exp(l0 - top), jnp.exp(l1 - top)
    gates[0] = jnp.broadcast_to(e0 / (e0 + e1), (tokens, 128))
    gates[1] = jnp.broadcast_to(e1 / (e0 + e1), (tokens, 128))

    def gather(src, pos, i):
        got = jnp.dot(sel_in[src], xall[src, i], preferred_element_type=f32).astype(bf16)
        for e in range(local):
            rows_buf[e, pos * cap:(pos + 1) * cap, cols(i)] = got[e * cap:(e + 1) * cap]

    pltpu.make_async_copy(sel_in.at[pl.ds(0, n_ep - 1)], sel_in.at[pl.ds(0, n_ep - 1)], sel_recv).wait()

    def own(i, carry):
        gather(me, 0, i)
        return carry

    lax.fori_loop(0, tiles, own, 0)

    def neighbours(i, carry):
        arrived(left, i)
        x_copy(left, i, partner, 4).start()

        @pl.when(lax.rem(i, 2) == 0)
        def _():
            x_copy(left, i, right, 3).start()

        gather(left, 2, i)
        arrived(right, i)
        x_copy(right, i, partner, 5).start()

        @pl.when(lax.rem(i, 2) == 1)
        def _():
            x_copy(right, i, left, 3).start()

        gather(right, 4, i)
        arrived(partner, i)
        gather(partner, 1, i)
        return carry

    lax.fori_loop(0, tiles, neighbours, 0)

    def neighbours2(i, carry):
        arrived(left2, i)
        gather(left2, 3, i)
        arrived(right2, i)
        gather(right2, 5, i)
        return carry

    lax.fori_loop(0, tiles, neighbours2, 0)

    def across(i, carry):
        arrived(far, i)
        x_copy(far, i, partner, 6).start()
        gather(far, 6, i)
        return carry

    def across2(i, carry):
        arrived(far2, i)
        gather(far2, 7, i)
        return carry

    block = 16

    def normalise(first, count):
        def step(r, carry):
            rows = pl.ds(pl.multiple_of(first + r * block, block), block)
            for e in range(local):
                acc = jnp.zeros((block, tile), f32)
                for i in range(tiles):
                    v = rows_buf[e, rows, i * tile:(i + 1) * tile].astype(f32)
                    acc = acc + v * v
                scale = lax.rsqrt(jnp.sum(acc, axis=1, keepdims=True) / d_model + NORM_EPS)
                for i in range(tiles):
                    span = slice(i * tile, (i + 1) * tile)
                    v = rows_buf[e, rows, span].astype(f32)
                    rows_buf[e, rows, span] = (v * scale * gains[:, span]).astype(bf16)
            return carry

        lax.fori_loop(0, count // block, step, 0)

    def expand(e):
        def narrow(lo, size):
            up_in = rows_buf[e]
            gate = lax.dot_general(up_in, gbuf[2 * e, pl.ds(lo, size), :], last, preferred_element_type=f32)
            up = lax.dot_general(up_in, gbuf[2 * e + 1, pl.ds(lo, size), :], last, preferred_element_type=f32)
            inner[:, pl.ds(lo, size)] = (jax.nn.silu(gate) * up).astype(bf16)

        def step(n, carry):
            narrow(pl.multiple_of(n * 128, 128), 128)
            return carry

        lax.fori_loop(0, d_ff // 128, step, 0)
        if d_ff % 128:
            narrow(d_ff // 128 * 128, d_ff % 128)

    def y_copy(e, i, pos):
        return pltpu.make_async_remote_copy(
            src_ref=rows_buf.at[e, pl.ds(pos * cap, cap), cols(i)],
            dst_ref=ret.at[pl.ds(pl.multiple_of((me * local + e) * cap, cap), cap), cols(i)],
            send_sem=ysend.at[e, i], recv_sem=yrecv.at[e, i],
            device_id={'ep': peers[pos]}, device_id_type=MESH_ID,
        )

    def contract(e):
        def step(i, carry):
            q = e * tiles + i
            wd_copy(q).wait()
            y = jnp.dot(inner[...], wdbuf[lax.rem(q, wd_slots)], preferred_element_type=f32).astype(bf16)

            @pl.when(q + wd_slots < wd_total)
            def _():
                wd_copy(q + wd_slots).start()

            rows_buf[e, :, cols(i)] = y
            ret[pl.ds(pl.multiple_of((me * local + e) * cap, cap), cap), cols(i)] = y[:cap]
            for pos in range(1, n_ep):
                y_copy(e, i, pos).start()
            return carry

        lax.fori_loop(0, tiles, step, 0)

    lax.fori_loop(0, tiles, across, 0)
    lax.fori_loop(0, tiles, across2, 0)
    normalise(0, n_ep * cap)
    for g in range(2 * local):
        ff_copy(g).wait()

    def serve(e, carry):
        expand(e)
        contract(e)
        return carry

    lax.fori_loop(0, local, serve, 0)

    whole = pl.ds(0, (n_ep - 1) * cap)

    def finish(i, carry):
        for e in range(local):
            pltpu.make_async_copy(ret.at[whole, cols(i)], ret.at[whole, cols(i)], yrecv.at[e, i]).wait()
        picked = jnp.dot(comb[...], ret[:, cols(i)], preferred_element_type=f32)
        reps = tile // 128
        g0 = jnp.concatenate([gates[0]] * reps, axis=1)
        g1 = jnp.concatenate([gates[1]] * reps, axis=1)
        out[:, cols(i)] = xall[me, i].astype(f32) + (g0 * picked[:tokens] + g1 * picked[tokens:])
        return carry

    lax.fori_loop(0, tiles, finish, 0)

    def drain(i, carry):
        for kind in (0, 1, 2, 3, 4, 5, 6):
            pltpu.make_async_copy(xall.at[0, i], xall.at[0, i], xsend.at[kind, i]).wait()
        for e in range(local):
            pltpu.make_async_copy(ret.at[whole, cols(i)], ret.at[whole, cols(i)], ysend.at[e, i]).wait()
        return carry

    lax.fori_loop(0, tiles, drain, 0)
    pltpu.make_async_copy(sel_in.at[pl.ds(0, n_ep - 1)], sel_in.at[pl.ds(0, n_ep - 1)], sel_send).wait()


def moe(mix, hidden, expert_ids, ffn_gain, w_out, w_router, w_gate, w_up, w_down, n_ep):
    tokens, d_model = hidden.shape
    local, _, d_ff = w_gate.shape
    n_experts = local * n_ep
    cap = 4 * tokens // n_experts
    tile = 512
    tiles = d_model // tile
    vmem = pl.BlockSpec(memory_space=pltpu.VMEM)
    hbm = pl.BlockSpec(memory_space=pl.ANY)
    dma = pltpu.SemaphoreType.DMA
    return pl.pallas_call(
        functools.partial(moe_kernel, n_ep=n_ep, tile=tile, cap=cap),
        out_shape=jax.ShapeDtypeStruct((tokens, d_model), jnp.float32),
        in_specs=[vmem] * 5 + [hbm] * 4,
        out_specs=vmem,
        scratch_shapes=[
            pltpu.VMEM((2 * local, d_ff, d_model), jnp.bfloat16),
            pltpu.VMEM((4, d_ff, tile), jnp.bfloat16),
            pltpu.VMEM((n_ep, tiles, tokens, tile), jnp.bfloat16),
            pltpu.VMEM((local, n_ep * cap, d_model), jnp.bfloat16),
            pltpu.VMEM((n_ep * cap, d_ff), jnp.bfloat16),
            pltpu.VMEM((n_experts * cap, d_model), jnp.bfloat16),
            pltpu.VMEM((n_ep, local * cap, tokens), jnp.bfloat16),
            pltpu.VMEM((n_ep, local * cap, tokens), jnp.bfloat16),
            pltpu.VMEM((2 * tokens, n_experts * cap), jnp.bfloat16),
            pltpu.VMEM((2, tokens, 128), jnp.float32),
            pltpu.VMEM((1, d_model), jnp.float32),
            dma((4,)), dma((4,)), dma((4,)),
            dma((7, tiles)), dma((n_ep, tiles)),
            dma, dma,
            dma((local, tiles)), dma((local, tiles)),
        ],
        compiler_params=pltpu.CompilerParams(collective_id=0, has_side_effects=True, vmem_limit_bytes=VMEM_LIMIT),
        name="moe",
    )(mix, hidden, expert_ids.T, ffn_gain.reshape(-1, 128), w_router.T, w_out, w_gate.transpose(0, 2, 1), w_up.transpose(0, 2, 1), w_down)


def packed_kernel(
    mix, hidden, ids_row, gain, router, wo, wg, wu, wd,
    out, fits,
    gbuf, wdbuf, xown, xmate, stage, xin, rows_buf, wide_acc, inner, ret, ycross, ystage,
    slots_out, slots_in, spread, own_sel, sel, pack, comb, gates, gains, scale_out, scale_in, row_scale,
    wo_sem, wg_sem, wd_sem, slot_send, slot_recv, near_send, far_send, mate_send, fwd_send, x_recv, mate_recv,
    ysend_mate, yrecv_mate, cross_send, cross_recv, ysend, yrecv, scale_send, scale_recv,
    *, n_ep, tile, cap, room,
):
    tokens, d_model = hidden.shape
    d_ff = wg.shape[1]
    local = wg.shape[0]
    n_experts = local * n_ep
    tiles = d_model // tile
    ring = n_ep // 2
    slab = local * cap
    chip_slab = 2 * slab
    f32, bf16 = jnp.float32, jnp.bfloat16
    last = (((1,), (1,)), ((), ()))

    me = lax.axis_index('ep')
    x, c = me // 2, lax.rem(me, 2)
    other = 1 - c

    def at(step, core):
        return lax.rem(x + step, ring) * 2 + core

    mate = at(0, other)
    places = [at(3, c), at(3, other), at(1, c), at(1, other), at(2, c), at(2, other)]
    peers = [mate] + places

    def cols(i):
        return pl.ds(pl.multiple_of(i * tile, tile), tile)

    def to(dev):
        return {'device_id': {'ep': dev}, 'device_id_type': MESH_ID}

    def landed(ref, sem):
        pltpu.make_async_copy(ref, ref, sem).wait()

    parts = d_model // tile

    def wo_start(i, slot):
        for j in range(parts):
            span = slice(j * tile, (j + 1) * tile)
            pltpu.make_async_copy(wo.at[span, cols(i)], gbuf.at[slot, 0:tile, span], wo_sem.at[slot]).start()

    def wo_wait(slot):
        pltpu.make_async_copy(wo.at[0:tile, :], gbuf.at[slot, 0:tile, :], wo_sem.at[slot]).wait()

    def ff_copy(g):
        src = wg if g % 2 == 0 else wu
        return pltpu.make_async_copy(src.at[g // 2], gbuf.at[g], wg_sem.at[g])

    wd_slots = wdbuf.shape[0]
    wd_total = local * tiles

    def tile_of(q):
        k = lax.rem(q // local, tiles)
        return 2 * (k // 2) + lax.rem(other + lax.rem(k, 2), 2)

    def wd_get(q):
        slot = lax.rem(q, wd_slots)
        return pltpu.make_async_copy(wd.at[lax.rem(q, local), :, cols(tile_of(q))], wdbuf.at[slot], wd_sem.at[slot])

    def wd_wait(q):
        wd_get(q).wait()

    def wd_next(q):
        @pl.when(q + wd_slots < wd_total)
        def _():
            wd_get(q + wd_slots).start()

    for i in range(4):
        wo_start(i, i)

    barrier = pltpu.get_barrier_semaphore()
    for peer in peers:
        pl.semaphore_signal(barrier, inc=1, device_id={'ep': peer}, device_id_type=MESH_ID)

    t_sub = lax.broadcasted_iota(jnp.int32, (tokens, tokens), 0)
    t_lane = lax.broadcasted_iota(jnp.int32, (tokens, tokens), 1)
    before = (t_sub < t_lane).astype(f32).astype(bf16)
    id0_row, id1_row = ids_row[0:1, :].astype(f32), ids_row[1:2, :].astype(f32)
    e_sub = lax.broadcasted_iota(jnp.int32, (n_experts, tokens), 0).astype(f32)
    spread_gain(gain, gains)
    hit_row = jnp.logical_or(e_sub == id0_row, e_sub == id1_row).astype(f32).astype(bf16)
    rank_row = jnp.dot(hit_row, before, preferred_element_type=f32)
    slots_row = []
    for ident in (id0_row, id1_row):
        rank = jnp.sum(jnp.where(e_sub == ident, rank_row, 0.0), axis=0, keepdims=True)
        slots_row.append(ident * cap + rank)
    eight = lax.broadcasted_iota(jnp.int32, (8, tokens), 0)
    slots_out[...] = jnp.where(eight == 0, slots_row[0], slots_row[1])

    def inside(slot, chip):
        low = (chip * chip_slab).astype(f32) if not isinstance(chip, int) else float(chip * chip_slab)
        return jnp.logical_and(slot >= low, slot < low + chip_slab).astype(f32)

    def ranks(s0, s1, chip):
        in0, in1 = inside(s0, chip), inside(s1, chip)
        uses = jnp.maximum(in0, in1)
        rows = jnp.where(eight == 0, uses, jnp.where(eight == 1, in0, in1))
        got = jnp.dot(rows.astype(bf16), before, preferred_element_type=f32)
        base = jnp.sum(in0, axis=1, keepdims=True)
        return in0, in1, uses, got[0:1, :], got[1:2, :], base + got[2:3, :]

    p_sub = lax.broadcasted_iota(jnp.int32, (room, tokens), 0).astype(f32)
    steps = (3, 1, 2)
    index = [jnp.zeros((1, tokens), f32), jnp.zeros((1, tokens), f32)]
    for k, step in enumerate(steps):
        in0, in1, uses, dpos, q0, q1 = ranks(slots_row[0], slots_row[1], lax.rem(x + step, ring))
        spread[k] = jnp.logical_and(p_sub == dpos, uses > 0.5).astype(f32).astype(bf16)
        index[0] = index[0] + in0 * (k * room + q0)
        index[1] = index[1] + in1 * (k * room + q1)
    mine_low = (x * chip_slab).astype(f32)
    for k in range(2):
        index[k] = index[k] + inside(slots_row[k], x) * (3 * room + slots_row[k] - mine_low)
    width = 3 * room + chip_slab
    w_lane = lax.broadcasted_iota(jnp.int32, (tokens, width), 1).astype(f32)
    for k in range(2):
        comb[k * tokens:(k + 1) * tokens, :] = (w_lane == column_of(index[k])[:, 0:1]).astype(f32).astype(bf16)

    def slot_sel(dev, s0, s1):
        want = (lax.broadcasted_iota(jnp.int32, (slab, tokens), 0) + dev * slab).astype(f32)
        return jnp.logical_or(want == s0, want == s1).astype(f32).astype(bf16)

    pl.semaphore_wait(barrier, n_ep - 1)
    for k, peer in enumerate(peers):
        there = (0, 3, 4, 1, 2, 5, 6)[k]
        pltpu.make_async_remote_copy(
            src_ref=slots_out, dst_ref=slots_in.at[there], send_sem=slot_send.at[k], recv_sem=slot_recv.at[there], **to(peer),
        ).start()

    def x_copy(place, i):
        k, dev, there = {0: (0, places[0], 2), 2: (1, places[2], 0), 4: (2, places[4], 4)}[place]
        sem = near_send.at[k, i] if k < 2 else far_send.at[i]
        return pltpu.make_async_remote_copy(
            src_ref=stage.at[k, i], dst_ref=xin.at[there, i], send_sem=sem, recv_sem=x_recv.at[there, i], **to(dev),
        )

    def mate_copy(i):
        return pltpu.make_async_remote_copy(
            src_ref=xown.at[i], dst_ref=xmate.at[i], send_sem=mate_send.at[i], recv_sem=mate_recv.at[i], **to(mate),
        )

    def fwd_copy(place, i):
        return pltpu.make_async_remote_copy(
            src_ref=xin.at[place, i], dst_ref=xin.at[place + 1, i], send_sem=fwd_send.at[place // 2, i],
            recv_sem=x_recv.at[place + 1, i], **to(mate),
        )

    own_sel[0] = slot_sel(me, slots_row[0], slots_row[1])
    c_lane = lax.broadcasted_iota(jnp.int32, (chip_slab, tokens), 0)
    want = (lax.rem(c_lane + c * slab, chip_slab) + x * chip_slab).astype(f32)

    def learn(k):
        landed(slots_in.at[k], slot_recv.at[k])
        s0, s1 = slots_in[k, 0:1, :], slots_in[k, 1:2, :]
        own_sel[k + 1] = slot_sel(me, s0, s1)
        in0, in1, uses, dpos, q0, q1 = ranks(s0, s1, x)
        put = jnp.logical_and(p_sub == dpos, uses > 0.5).astype(f32).astype(bf16)
        sel[k] = lax.dot_general(own_sel[k + 1], put, last, preferred_element_type=f32).astype(bf16)
        total = jnp.zeros((room, chip_slab), f32)
        for s, inn, q in ((s0, in0, q0), (s1, in1, q1)):
            spot = jnp.logical_and(p_sub == q, inn > 0.5).astype(f32).astype(bf16)
            total = total + lax.dot_general(spot, (want == s).astype(f32).astype(bf16), last, preferred_element_type=f32)
        pack[k] = total.astype(bf16)

    def project(i, carry):
        slot = lax.rem(i, 4)
        wo_wait(slot)
        acc = jnp.zeros((tokens, tile), f32)
        for j in range(parts):
            span = slice(j * tile, (j + 1) * tile)
            acc = acc + jnp.dot(mix[:, span], gbuf[slot, 0:tile, span], preferred_element_type=f32)
        xt = (hidden[:, cols(i)].astype(f32) + acc).astype(bf16)
        xown[i] = xt
        for k in range(3):
            stage[k, i] = jnp.dot(spread[k], xt, preferred_element_type=f32).astype(bf16)
        x_copy(0, i).start()
        x_copy(2, i).start()
        mate_copy(i).start()

        @pl.when(i < n_ep - 1)
        def _():
            learn(i)

        wide = xt.astype(f32)
        wide = wide * wide
        for j in range(0, tile, 128):
            carry = carry + wide[:, j:j + 128]

        @pl.when(i < 4)
        def _():
            wo_start(i + 4, slot)

        for g in range(4):
            @pl.when(i == g + 4)
            def _():
                ff_copy(g).start()
        return carry

    sums = lax.fori_loop(0, tiles, project, jnp.zeros((tokens, 128), f32))
    inv = lax.rsqrt(jnp.sum(sums, axis=1, keepdims=True) / d_model + NORM_EPS)
    inv_row = jnp.broadcast_to(inv, (tokens, 128)).T[0:8, :]
    scale_out[...] = inv_row
    for k, peer in enumerate(peers):
        there = (0, 3, 4, 1, 2, 5, 6)[k]
        pltpu.make_async_remote_copy(
            src_ref=scale_out, dst_ref=scale_in.at[there], send_sem=scale_send.at[k], recv_sem=scale_recv.at[there], **to(peer),
        ).start()

    def send_far(i, carry):
        x_copy(4, i).start()
        return carry

    lax.fori_loop(0, tiles, send_far, 0)
    for q in range(wd_slots):
        wd_get(jnp.int32(q)).start()

    def learn_scale(k, row):
        hit = own_sel[k].astype(f32) * row
        row_scale[k] = jnp.broadcast_to(jnp.sum(hit, axis=1, keepdims=True), (slab, 128))

    def gather(pick, block, pos, i):
        got = jnp.dot(pick, block, preferred_element_type=f32)
        mul = jnp.concatenate([row_scale[pos]] * (tile // 128), axis=1)
        got = (got * mul * gains[:, cols(i)]).astype(bf16)
        for e in range(local):
            rows_buf[e, pos * cap:(pos + 1) * cap, cols(i)] = got[e * cap:(e + 1) * cap]

    def scale_from(k):
        landed(scale_in.at[k], scale_recv.at[k])
        learn_scale(k + 1, scale_in[k, 0:1, :])

    learn_scale(0, inv_row[0:1, :])
    scale_from(0)

    def own(i, carry):
        landed(xmate.at[i], mate_recv.at[i])
        gather(own_sel[0], xown[i], 0, i)
        gather(own_sel[1], xmate[i], 1, i)
        for place in (0, 2):
            landed(xin.at[place, i], x_recv.at[place, i])
            fwd_copy(place, i).start()
        return carry

    lax.fori_loop(0, tiles, own, 0)
    for k in range(1, 5):
        scale_from(k)

    def neighbours(i, carry):
        for place in (1, 3):
            landed(xin.at[place, i], x_recv.at[place, i])
        for place in range(4):
            gather(sel[place + 1], xin[place, i], place + 2, i)
        return carry

    lax.fori_loop(0, tiles, neighbours, 0)
    for k in range(5, 7):
        scale_from(k)

    for g in range(2 * local):
        ff_copy(g).wait()

    def expand(i):
        for e in range(local):
            for k in range(2):
                part = lax.dot_general(rows_buf[e, :, cols(i)], gbuf[2 * e + k, :, cols(i)], last, preferred_element_type=f32)
                wide_acc[2 * e + k] = jnp.where(i == 0, part, wide_acc[2 * e + k] + part)

    def last_source(i):
        landed(xin.at[5, i], x_recv.at[5, i])
        gather(sel[6], xin[5, i], 7, i)
        expand(i)

    def across(i, carry):
        landed(xin.at[4, i], x_recv.at[4, i])
        fwd_copy(4, i).start()
        gather(sel[5], xin[4, i], 6, i)

        @pl.when(i > 0)
        def _():
            last_source(i - 1)
        return carry

    lax.fori_loop(0, tiles, across, 0)
    last_source(tiles - 1)
    for e in range(local):
        inner[e] = (jax.nn.silu(wide_acc[2 * e]) * wide_acc[2 * e + 1]).astype(bf16)


    def mate_y(e, i):
        return pltpu.make_async_remote_copy(
            src_ref=rows_buf.at[e, pl.ds(cap, cap), cols(i)],
            dst_ref=ret.at[pl.ds(pl.multiple_of(3 * room + c * slab + e * cap, cap // 2), cap), cols(i)],
            send_sem=ysend_mate.at[e, i], recv_sem=yrecv_mate.at[e, i], **to(mate),
        )

    lead = 2 * cap

    def cross_y(e, i):
        rows = pl.ds(lead, n_ep * cap - lead)
        return pltpu.make_async_remote_copy(
            src_ref=rows_buf.at[e, rows, cols(i)], dst_ref=ycross.at[i // 2, e, rows],
            send_sem=cross_send.at[e, i // 2], recv_sem=cross_recv.at[e, i // 2], **to(mate),
        )

    def y_copy(place, half, i):
        there = (1, 1, 0, 0, 2, 2)[place]
        return pltpu.make_async_remote_copy(
            src_ref=ystage.at[place, half], dst_ref=ret.at[pl.ds(there * room, room), cols(i)],
            send_sem=ysend.at[place, half], recv_sem=yrecv.at[there, i], **to(places[place]),
        )

    def contract():
        def finish_pair(half):
            i = 2 * half + c
            for e in range(local):
                landed(ycross.at[half, e, pl.ds(lead, n_ep * cap - lead)], cross_recv.at[e, half])
            for pos in range(2, n_ep):
                block_rows = slice(pos * cap, (pos + 1) * cap)
                swapped = slice((pos ^ 1) * cap, ((pos ^ 1) + 1) * cap)
                pieces = [rows_buf[e, block_rows, cols(i)] for e in range(local)] + [ycross[half, e, swapped, :] for e in range(local)]
                ystage[pos - 2, half] = jnp.dot(pack[pos - 1], jnp.concatenate(pieces, axis=0), preferred_element_type=f32).astype(bf16)
                y_copy(pos - 2, half, i).start()

        def pair(half, carry):
            for k in range(2):
                i = 2 * half + (lax.rem(other + k, 2))
                for e in range(local):
                    q = (2 * half + k) * local + e
                    wd_wait(q)
                    y = jnp.dot(inner[e], wdbuf[lax.rem(q, wd_slots)], preferred_element_type=f32).astype(bf16)
                    wd_next(q)
                    rows_buf[e, :, cols(i)] = y
                    if k == 0:
                        cross_y(e, i).start()
                    ret[pl.ds(pl.multiple_of(3 * room + c * slab + e * cap, cap // 2), cap), cols(i)] = y[:cap]
                    mate_y(e, i).start()

            @pl.when(half > 0)
            def _():
                finish_pair(half - 1)
            return carry

        lax.fori_loop(0, tiles // 2, pair, 0)
        finish_pair(tiles // 2 - 1)

    contract()

    top = jnp.zeros((1, 1), f32)
    for s0, s1 in [(slots_row[0], slots_row[1])] + [(slots_in[k, 0:1, :], slots_in[k, 1:2, :]) for k in range(n_ep - 1)]:
        for d in range(ring):
            top = jnp.maximum(top, jnp.sum(inside(s0, d) + inside(s1, d), axis=1, keepdims=True))
    fits[0] = (top[0, 0] <= room).astype(jnp.int32)

    def route(i, acc):
        v = (xown[i].astype(f32) * inv * gains[:, cols(i)]).astype(bf16)
        return acc + lax.dot_general(v, router[:, cols(i)], last, preferred_element_type=f32)

    logits = lax.fori_loop(0, tiles, route, jnp.zeros((tokens, n_experts), f32))
    e_lane = lax.broadcasted_iota(jnp.int32, (tokens, n_experts), 1).astype(f32)
    id0, id1 = column_of(id0_row)[:, 0:1], column_of(id1_row)[:, 0:1]
    l0 = jnp.sum(jnp.where(e_lane == id0, logits, 0.0), axis=1, keepdims=True)
    l1 = jnp.sum(jnp.where(e_lane == id1, logits, 0.0), axis=1, keepdims=True)
    top = jnp.maximum(l0, l1)
    e0, e1 = jnp.exp(l0 - top), jnp.exp(l1 - top)
    gates[0] = jnp.broadcast_to(e0 / (e0 + e1), (tokens, 128))
    gates[1] = jnp.broadcast_to(e1 / (e0 + e1), (tokens, 128))

    def finish(i, carry):
        for e in range(local):
            landed(ret.at[pl.ds(0, cap), cols(i)], yrecv_mate.at[e, i])
        for k in range(3):
            landed(ret.at[pl.ds(0, room), cols(i)], yrecv.at[k, i])
        picked = jnp.dot(comb[...], ret[:, cols(i)], preferred_element_type=f32)
        reps = tile // 128
        g0 = jnp.concatenate([gates[0]] * reps, axis=1)
        g1 = jnp.concatenate([gates[1]] * reps, axis=1)
        out[:, cols(i)] = xown[i].astype(f32) + (g0 * picked[:tokens] + g1 * picked[tokens:])
        return carry

    lax.fori_loop(0, tiles, finish, 0)

    def drain(i, carry):
        for k in range(2):
            landed(stage.at[0, 0], near_send.at[k, i])
        landed(stage.at[0, 0], far_send.at[i])
        landed(xown.at[0], mate_send.at[i])
        for k in range(3):
            landed(stage.at[0, 0], fwd_send.at[k, i])
        for e in range(local):
            landed(ret.at[pl.ds(0, cap), cols(0)], ysend_mate.at[e, i])
        return carry

    lax.fori_loop(0, tiles, drain, 0)

    def drain2(half, carry):
        for e in range(local):
            landed(ycross.at[0, 0, pl.ds(lead, n_ep * cap - lead)], cross_send.at[e, half])
        for place in range(6):
            landed(ystage.at[0, 0], ysend.at[place, half])
        return carry

    lax.fori_loop(0, tiles // 2, drain2, 0)
    for k in range(7):
        landed(slots_out, slot_send.at[k])
        landed(scale_out, scale_send.at[k])


def moe_packed(mix, hidden, expert_ids, ffn_gain, w_out, w_router, w_gate, w_up, w_down, n_ep, room):
    tokens, d_model = hidden.shape
    local, _, d_ff = w_gate.shape
    n_experts = local * n_ep
    cap = 4 * tokens // n_experts
    slab = local * cap
    tile = 512
    tiles = d_model // tile
    vmem = pl.BlockSpec(memory_space=pltpu.VMEM)
    hbm = pl.BlockSpec(memory_space=pl.ANY)
    dma = pltpu.SemaphoreType.DMA
    bf16 = jnp.bfloat16
    return pl.pallas_call(
        functools.partial(packed_kernel, n_ep=n_ep, tile=tile, cap=cap, room=room),
        out_shape=(jax.ShapeDtypeStruct((tokens, d_model), jnp.float32), jax.ShapeDtypeStruct((1,), jnp.int32)),
        in_specs=[vmem] * 5 + [hbm] * 4,
        out_specs=(vmem, pl.BlockSpec(memory_space=pltpu.SMEM)),
        scratch_shapes=[
            pltpu.VMEM((2 * local, d_ff, d_model), bf16),
            pltpu.VMEM((4, d_ff, tile), bf16),
            pltpu.VMEM((tiles, tokens, tile), bf16),
            pltpu.VMEM((tiles, tokens, tile), bf16),
            pltpu.VMEM((3, tiles, room, tile), bf16),
            pltpu.VMEM((6, tiles, room, tile), bf16),
            pltpu.VMEM((local, n_ep * cap, d_model), bf16),
            pltpu.VMEM((2 * local, n_ep * cap, d_ff), jnp.float32),
            pltpu.VMEM((local, n_ep * cap, d_ff), bf16),
            pltpu.VMEM((3 * room + 2 * slab, d_model), bf16),
            pltpu.VMEM((tiles // 2, local, n_ep * cap, tile), bf16),
            pltpu.VMEM((6, tiles // 2, room, tile), bf16),
            pltpu.VMEM((8, tokens), jnp.float32),
            pltpu.VMEM((7, 8, tokens), jnp.float32),
            pltpu.VMEM((3, room, tokens), bf16),
            pltpu.VMEM((n_ep, slab, tokens), bf16),
            pltpu.VMEM((n_ep - 1, slab, room), bf16),
            pltpu.VMEM((n_ep - 1, room, 2 * slab), bf16),
            pltpu.VMEM((2 * tokens, 3 * room + 2 * slab), bf16),
            pltpu.VMEM((2, tokens, 128), jnp.float32),
            pltpu.VMEM((1, d_model), jnp.float32),
            pltpu.VMEM((8, tokens), jnp.float32),
            pltpu.VMEM((n_ep - 1, 8, tokens), jnp.float32),
            pltpu.VMEM((n_ep, slab, 128), jnp.float32),
            dma((4,)), dma((4,)), dma((4,)),
            dma((7,)), dma((7,)),
            dma((2, tiles)), dma((tiles,)), dma((tiles,)), dma((3, tiles)), dma((6, tiles)), dma((tiles,)),
            dma((local, tiles)), dma((local, tiles)),
            dma((local, tiles // 2)), dma((local, tiles // 2)),
            dma((6, tiles // 2)), dma((3, tiles)),
            dma((n_ep - 1,)), dma((n_ep - 1,)),
        ],
        compiler_params=pltpu.CompilerParams(collective_id=1, has_side_effects=True, vmem_limit_bytes=VMEM_LIMIT),
        name="moe_packed",
    )(mix, hidden, expert_ids.T, ffn_gain.reshape(-1, 128), w_router.T, w_out, w_gate.transpose(0, 2, 1), w_up.transpose(0, 2, 1), w_down)


def solution(mesh):
    n_ep = mesh.shape['ep']
    row_spec = P(('dp', 'ep'), None)
    cache_spec = P(('dp', 'ep'), None, None, None)
    expert_spec = P('ep', None, None)
    in_specs = (row_spec, cache_spec, cache_spec, P(('dp', 'ep')), row_spec, P(), P(), P(), P(), P(), P(), P(), expert_spec, expert_spec, expert_spec)
    out_specs = (row_spec, cache_spec, cache_spec)

    def device_step(hidden, k_cache, v_cache, seq_lens, expert_ids, attn_gain, w_query, w_key, w_value, w_out, ffn_gain, w_router, w_gate, w_up, w_down):
        mix, k_cache_new, v_cache_new = attention(hidden, k_cache, v_cache, seq_lens, attn_gain, w_query, w_key, w_value)
        operands = (mix, hidden, expert_ids, ffn_gain, w_out, w_router, w_gate, w_up, w_down)
        room = 5 * hidden.shape[0] // 8
        out, fits = moe_packed(*operands, n_ep, room)
        out = lax.cond(fits[0] == 1, lambda ops: ops[0].astype(jnp.bfloat16), lambda ops: moe(*ops[1:], n_ep).astype(jnp.bfloat16), (out,) + operands)
        return out, k_cache_new, v_cache_new

    return jax.shard_map(device_step, mesh=mesh, in_specs=in_specs, out_specs=out_specs, check_vma=False)
```

```python
import functools

import jax
import jax.numpy as jnp
import numpy as np
from jax import lax
from jax.experimental import pallas as pl
from jax.experimental.pallas import tpu as pltpu
from jax.sharding import PartitionSpec as P

NORM_EPS = 1e-5
ROPE_THETA = 1000000.0
VMEM_LIMIT = 67000000


def spread_gain(gain, gains):
    lanes = gain.shape[1]
    wide = gain[...].astype(jnp.float32)
    for r in range(gain.shape[0]):
        gains[:, r * lanes:(r + 1) * lanes] = wide[r:r + 1, :]


def column_of(row):
    return jnp.broadcast_to(row, (row.shape[1], row.shape[1])).T


def attn_kernel(
    lens, hidden, gain, lens_row, freq, wq, wk, wv, kc, vc,
    mix, kn, vn,
    normed, wbuf, kbuf, vbuf, heads, mixed, cos, sin, gains, wsem, ksem, vsem, kout, vout,
    *, kv_heads, tile, chunk,
):
    tokens, d_model = hidden.shape
    seq_len, head_dim = kc.shape[1], kc.shape[3]
    q_tiles, kv_tiles = wq.shape[1] // tile, wk.shape[1] // tile
    n_tiles = q_tiles + 2 * kv_tiles
    per_tile = tile // head_dim
    q_heads = wq.shape[1] // head_dim
    groups = q_heads // kv_heads
    pitch = tokens + 8
    slots = wbuf.shape[0]
    n_chunks = tokens // chunk

    def fetch(i, slot):
        @pl.when(i < q_tiles)
        def _():
            pltpu.make_async_copy(wq.at[:, pl.ds(pl.multiple_of(i * tile, tile), tile)], wbuf.at[slot], wsem.at[slot]).start()

        @pl.when(jnp.logical_and(i >= q_tiles, i < q_tiles + kv_tiles))
        def _():
            pltpu.make_async_copy(wk.at[:, pl.ds(pl.multiple_of((i - q_tiles) * tile, tile), tile)], wbuf.at[slot], wsem.at[slot]).start()

        @pl.when(jnp.logical_and(i >= q_tiles + kv_tiles, i < n_tiles))
        def _():
            pltpu.make_async_copy(wv.at[:, pl.ds(pl.multiple_of((i - q_tiles - kv_tiles) * tile, tile), tile)], wbuf.at[slot], wsem.at[slot]).start()

    def rows(c):
        return pl.ds(pl.multiple_of(c * chunk, chunk), chunk)

    for i in range(slots):
        fetch(jnp.int32(i), i)

    spread_gain(gain, gains)
    x = hidden[...].astype(jnp.float32)
    inv = lax.rsqrt(jnp.mean(x * x, axis=-1, keepdims=True) + NORM_EPS)
    normed[...] = (x * inv * gains[...]).astype(jnp.bfloat16)
    angles = column_of(lens_row[...].astype(jnp.float32)) * freq[...]
    sines = jnp.sin(angles)
    lane = lax.broadcasted_iota(jnp.int32, angles.shape, 1)
    cos[...] = jnp.cos(angles)
    sin[...] = jnp.where(lane < head_dim // 2, -sines, sines)

    def project(i, carry):
        slot = lax.rem(i, slots)
        pltpu.make_async_copy(wq.at[:, pl.ds(0, tile)], wbuf.at[slot], wsem.at[slot]).wait()
        out = jnp.dot(normed[...], wbuf[slot], preferred_element_type=jnp.float32)
        fetch(i + slots, slot)

        @pl.when(i + slots == n_tiles)
        def _():
            def start(c, carry):
                pltpu.make_async_copy(kc.at[rows(c)], kbuf.at[rows(c)], ksem.at[c]).start()
                pltpu.make_async_copy(vc.at[rows(c)], vbuf.at[rows(c)], vsem.at[c]).start()
                return carry

            lax.fori_loop(0, n_chunks, start, 0)

        turn = i < q_tiles + kv_tiles
        c_val = jnp.where(turn, cos[...], 1.0)
        s_val = jnp.where(turn, sin[...], 0.0)
        for j in range(per_tile):
            block = out[:, j * head_dim:(j + 1) * head_dim].astype(jnp.bfloat16).astype(jnp.float32)
            block = block * c_val + pltpu.roll(block, head_dim // 2, axis=1) * s_val
            block = block.astype(jnp.bfloat16).astype(jnp.float32)
            heads[pl.ds(pl.multiple_of((i * per_tile + j) * pitch, 8), tokens), :] = block
        return carry

    lax.fori_loop(0, n_tiles, project, 0)

    head_of = lax.broadcasted_iota(jnp.int32, (q_heads, seq_len * kv_heads), 0) // groups
    column = lax.broadcasted_iota(jnp.int32, (q_heads, seq_len * kv_heads), 1)
    own = head_of == lax.rem(column, kv_heads)

    def attend(c, carry):
        pltpu.make_async_copy(kc.at[rows(c)], kbuf.at[rows(c)], ksem.at[c]).wait()
        pltpu.make_async_copy(vc.at[rows(c)], vbuf.at[rows(c)], vsem.at[c]).wait()
        base = c * chunk
        for j in range(chunk):
            t = base + j
            n = lens[t]
            kbuf[t, n] = heads[pl.ds(q_heads * pitch + t, kv_heads, stride=pitch), :].astype(jnp.bfloat16)
            vbuf[t, n] = heads[pl.ds((q_heads + kv_heads) * pitch + t, kv_heads, stride=pitch), :].astype(jnp.bfloat16)
        pltpu.make_async_copy(kbuf.at[rows(c)], kn.at[rows(c)], kout.at[c]).start()
        pltpu.make_async_copy(vbuf.at[rows(c)], vn.at[rows(c)], vout.at[c]).start()
        probs = []
        for j in range(chunk):
            t = base + j
            q = heads[pl.ds(t, q_heads, stride=pitch), :].astype(jnp.bfloat16)
            keys = kbuf[t].reshape(seq_len * kv_heads, head_dim)
            score = lax.dot_general(q, keys, (((1,), (1,)), ((), ())), preferred_element_type=jnp.float32)
            score = score * head_dim ** -0.5
            seen = jnp.logical_and(own, column < (lens[t] + 1) * kv_heads)
            score = jnp.where(seen, score, -jnp.inf)
            e = jnp.exp(score - jnp.max(score, axis=-1, keepdims=True))
            probs.append((e / jnp.sum(e, axis=-1, keepdims=True)).astype(jnp.bfloat16))
        for j in range(chunk):
            t = base + j
            values = vbuf[t].reshape(seq_len * kv_heads, head_dim)
            o = jnp.dot(probs[j], values, preferred_element_type=jnp.float32)
            mixed[pl.ds(t, q_heads, stride=pitch), :] = o
        return carry

    lax.fori_loop(0, n_chunks, attend, 0)

    for h in range(q_heads):
        mix[:, h * head_dim:(h + 1) * head_dim] = mixed[h * pitch:h * pitch + tokens, :].astype(jnp.bfloat16)

    def drain(c, carry):
        pltpu.make_async_copy(kbuf.at[rows(c)], kn.at[rows(c)], kout.at[c]).wait()
        pltpu.make_async_copy(vbuf.at[rows(c)], vn.at[rows(c)], vout.at[c]).wait()
        return carry

    lax.fori_loop(0, n_chunks, drain, 0)


def attention(hidden, k_cache, v_cache, seq_lens, attn_gain, w_query, w_key, w_value):
    tokens, seq_len, kv_heads, head_dim = k_cache.shape
    d_model = hidden.shape[1]
    n_heads = w_query.shape[1] // head_dim
    all_heads = n_heads + 2 * kv_heads
    half = head_dim // 2
    inv_freq = np.float32(ROPE_THETA) ** (np.float32(-2.0) * np.arange(half, dtype=np.float32) / np.float32(head_dim))
    freq = jnp.asarray(np.concatenate([inv_freq, inv_freq])[None], jnp.float32)
    tile, chunk, slots = 512, 16, 3
    n_chunks = tokens // chunk
    vmem = pl.BlockSpec(memory_space=pltpu.VMEM)
    hbm = pl.BlockSpec(memory_space=pl.ANY)
    return pl.pallas_call(
        functools.partial(attn_kernel, kv_heads=kv_heads, tile=tile, chunk=chunk),
        out_shape=(
            jax.ShapeDtypeStruct((tokens, n_heads * head_dim), jnp.bfloat16),
            jax.ShapeDtypeStruct(k_cache.shape, jnp.bfloat16),
            jax.ShapeDtypeStruct(v_cache.shape, jnp.bfloat16),
        ),
        in_specs=[pl.BlockSpec(memory_space=pltpu.SMEM)] + [vmem] * 4 + [hbm] * 5,
        out_specs=(vmem, hbm, hbm),
        scratch_shapes=[
            pltpu.VMEM((tokens, d_model), jnp.bfloat16),
            pltpu.VMEM((slots, d_model, tile), jnp.bfloat16),
            pltpu.VMEM(k_cache.shape, jnp.bfloat16),
            pltpu.VMEM(v_cache.shape, jnp.bfloat16),
            pltpu.VMEM((all_heads * (tokens + 8), head_dim), jnp.float32),
            pltpu.VMEM((n_heads * (tokens + 8), head_dim), jnp.float32),
            pltpu.VMEM((tokens, head_dim), jnp.float32),
            pltpu.VMEM((tokens, head_dim), jnp.float32),
            pltpu.VMEM((1, d_model), jnp.float32),
            pltpu.SemaphoreType.DMA((slots,)),
            pltpu.SemaphoreType.DMA((n_chunks,)),
            pltpu.SemaphoreType.DMA((n_chunks,)),
            pltpu.SemaphoreType.DMA((n_chunks,)),
            pltpu.SemaphoreType.DMA((n_chunks,)),
        ],
        compiler_params=pltpu.CompilerParams(vmem_limit_bytes=VMEM_LIMIT),
        name="attend",
    )(seq_lens, hidden, attn_gain.reshape(-1, 128), seq_lens.reshape(1, tokens), freq, w_query, w_key, w_value, k_cache, v_cache)


MESH_ID = pl.DeviceIdType.MESH


def moe_kernel(
    mix, hidden, ids_row, gain, router, wo, wg, wu, wd,
    out,
    gbuf, wdbuf, xall, rows_buf, inner, ret, sel_out, sel_in, comb, gates, gains,
    wo_sem, wg_sem, wd_sem, xsend, xrecv, sel_send, sel_recv, ysend, yrecv,
    *, n_ep, tile, cap,
):
    tokens, d_model = hidden.shape
    d_ff = wg.shape[1]
    local = wg.shape[0]
    n_experts = local * n_ep
    tiles = d_model // tile
    ring = n_ep // 2
    slab = local * cap
    f32, bf16 = jnp.float32, jnp.bfloat16
    last = (((1,), (1,)), ((), ()))

    me = lax.axis_index('ep')
    x, c = me // 2, lax.rem(me, 2)

    def at(step, core):
        return lax.rem(x + step, ring) * 2 + core

    other = 1 - c
    peers = [me, at(0, other), at(ring - 1, c), at(ring - 1, other), at(1, c), at(1, other), at(2, c), at(2, other)]
    partner, left, left2, right, right2, far, far2 = peers[1:]

    def cols(i):
        return pl.ds(pl.multiple_of(i * tile, tile), tile)

    parts = d_model // tile

    def wo_start(i, slot):
        for j in range(parts):
            span = slice(j * tile, (j + 1) * tile)
            pltpu.make_async_copy(wo.at[span, cols(i)], gbuf.at[slot, 0:tile, span], wo_sem.at[slot]).start()

    def wo_wait(slot):
        pltpu.make_async_copy(wo.at[0:tile, :], gbuf.at[slot, 0:tile, :], wo_sem.at[slot]).wait()

    def ff_copy(g):
        src = wg if g % 2 == 0 else wu
        return pltpu.make_async_copy(src.at[g // 2], gbuf.at[g], wg_sem.at[g])

    wd_slots = wdbuf.shape[0]
    wd_total = local * tiles

    def wd_copy(q):
        e = lax.rem(q // tiles, local)
        slot = lax.rem(q, wd_slots)
        return pltpu.make_async_copy(wd.at[e, :, cols(lax.rem(q, tiles))], wdbuf.at[slot], wd_sem.at[slot])

    for i in range(4):
        wo_start(i, i)

    barrier = pltpu.get_barrier_semaphore()
    for peer in peers[1:]:
        pl.semaphore_signal(barrier, inc=1, device_id={'ep': peer}, device_id_type=MESH_ID)
    pl.semaphore_wait(barrier, n_ep - 1)

    t_sub = lax.broadcasted_iota(jnp.int32, (tokens, tokens), 0)
    t_lane = lax.broadcasted_iota(jnp.int32, (tokens, tokens), 1)
    id0_row, id1_row = ids_row[0:1, :].astype(f32), ids_row[1:2, :].astype(f32)
    e_sub = lax.broadcasted_iota(jnp.int32, (n_experts, tokens), 0).astype(f32)
    spread_gain(gain, gains)
    hit_row = jnp.logical_or(e_sub == id0_row, e_sub == id1_row).astype(f32).astype(bf16)
    rank_row = jnp.dot(hit_row, (t_sub < t_lane).astype(f32).astype(bf16), preferred_element_type=f32)
    slots_row = []
    for ident in (id0_row, id1_row):
        rank = jnp.sum(jnp.where(e_sub == ident, rank_row, 0.0), axis=0, keepdims=True)
        slots_row.append(ident * cap + rank)
    for d in range(n_ep):
        want = (lax.broadcasted_iota(jnp.int32, (slab, tokens), 0) + d * slab).astype(f32)
        pick = jnp.logical_or(want == slots_row[0], want == slots_row[1])
        sel_out[d] = pick.astype(f32).astype(bf16)
    for k in range(1, n_ep):
        pltpu.make_async_remote_copy(
            src_ref=sel_out.at[peers[k]], dst_ref=sel_in.at[me], send_sem=sel_send, recv_sem=sel_recv,
            device_id={'ep': peers[k]}, device_id_type=MESH_ID,
        ).start()
    sel_in[me] = sel_out[me]

    id0, id1 = column_of(id0_row)[:, 0:1], column_of(id1_row)[:, 0:1]
    e_lane = lax.broadcasted_iota(jnp.int32, (tokens, n_experts), 1).astype(f32)
    hit = jnp.logical_or(e_lane == id0, e_lane == id1).astype(f32).astype(bf16)
    rank_col = jnp.dot((t_lane < t_sub).astype(f32).astype(bf16), hit, preferred_element_type=f32)
    s_lane = lax.broadcasted_iota(jnp.int32, (tokens, n_experts * cap), 1).astype(f32)
    for k, ident in enumerate((id0, id1)):
        rank = jnp.sum(jnp.where(e_lane == ident, rank_col, 0.0), axis=1, keepdims=True)
        comb[k * tokens:(k + 1) * tokens, :] = (s_lane == ident * cap + rank).astype(f32).astype(bf16)

    def x_copy(src, i, dev, kind):
        return pltpu.make_async_remote_copy(
            src_ref=xall.at[src, i], dst_ref=xall.at[src, i], send_sem=xsend.at[kind, i], recv_sem=xrecv.at[src, i],
            device_id={'ep': dev}, device_id_type=MESH_ID,
        )

    def arrived(src, i):
        pltpu.make_async_copy(xall.at[src, i], xall.at[src, i], xrecv.at[src, i]).wait()

    def project(i, carry):
        slot = lax.rem(i, 4)
        wo_wait(slot)
        acc = jnp.zeros((tokens, tile), f32)
        for j in range(parts):
            span = slice(j * tile, (j + 1) * tile)
            acc = acc + jnp.dot(mix[:, span], gbuf[slot, 0:tile, span], preferred_element_type=f32)
        xall[me, i] = (hidden[:, cols(i)].astype(f32) + acc).astype(bf16)
        x_copy(me, i, right, 0).start()
        x_copy(me, i, left, 1).start()
        x_copy(me, i, partner, 2).start()

        @pl.when(i < 4)
        def _():
            wo_start(i + 4, slot)

        for g in range(4):
            @pl.when(i == g + 4)
            def _():
                ff_copy(g).start()
        return carry

    lax.fori_loop(0, tiles, project, 0)
    for q in range(wd_slots):
        wd_copy(jnp.int32(q)).start()

    def square(i, acc):
        v = xall[me, i].astype(f32)
        return acc + jnp.sum(v * v, axis=1, keepdims=True)

    inv = lax.rsqrt(lax.fori_loop(0, tiles, square, jnp.zeros((tokens, 1), f32)) / d_model + NORM_EPS)

    def route(i, acc):
        v = (xall[me, i].astype(f32) * inv * gains[:, cols(i)]).astype(bf16)
        return acc + lax.dot_general(v, router[:, cols(i)], last, preferred_element_type=f32)

    logits = lax.fori_loop(0, tiles, route, jnp.zeros((tokens, n_experts), f32))
    l0 = jnp.sum(jnp.where(e_lane == id0, logits, 0.0), axis=1, keepdims=True)
    l1 = jnp.sum(jnp.where(e_lane == id1, logits, 0.0), axis=1, keepdims=True)
    top = jnp.maximum(l0, l1)
    e0, e1 = jnp.exp(l0 - top), jnp.exp(l1 - top)
    gates[0] = jnp.broadcast_to(e0 / (e0 + e1), (tokens, 128))
    gates[1] = jnp.broadcast_to(e1 / (e0 + e1), (tokens, 128))

    def gather(src, pos, i):
        got = jnp.dot(sel_in[src], xall[src, i], preferred_element_type=f32).astype(bf16)
        for e in range(local):
            rows_buf[e, pos * cap:(pos + 1) * cap, cols(i)] = got[e * cap:(e + 1) * cap]

    pltpu.make_async_copy(sel_in.at[pl.ds(0, n_ep - 1)], sel_in.at[pl.ds(0, n_ep - 1)], sel_recv).wait()

    def own(i, carry):
        gather(me, 0, i)
        return carry

    lax.fori_loop(0, tiles, own, 0)

    def neighbours(i, carry):
        arrived(left, i)
        x_copy(left, i, partner, 4).start()

        @pl.when(lax.rem(i, 2) == 0)
        def _():
            x_copy(left, i, right, 3).start()

        gather(left, 2, i)
        arrived(right, i)
        x_copy(right, i, partner, 5).start()

        @pl.when(lax.rem(i, 2) == 1)
        def _():
            x_copy(right, i, left, 3).start()

        gather(right, 4, i)
        arrived(partner, i)
        gather(partner, 1, i)
        return carry

    lax.fori_loop(0, tiles, neighbours, 0)

    def neighbours2(i, carry):
        arrived(left2, i)
        gather(left2, 3, i)
        arrived(right2, i)
        gather(right2, 5, i)
        return carry

    lax.fori_loop(0, tiles, neighbours2, 0)

    def across(i, carry):
        arrived(far, i)
        x_copy(far, i, partner, 6).start()
        gather(far, 6, i)
        return carry

    def across2(i, carry):
        arrived(far2, i)
        gather(far2, 7, i)
        return carry

    block = 16

    def normalise(first, count):
        def step(r, carry):
            rows = pl.ds(pl.multiple_of(first + r * block, block), block)
            for e in range(local):
                acc = jnp.zeros((block, tile), f32)
                for i in range(tiles):
                    v = rows_buf[e, rows, i * tile:(i + 1) * tile].astype(f32)
                    acc = acc + v * v
                scale = lax.rsqrt(jnp.sum(acc, axis=1, keepdims=True) / d_model + NORM_EPS)
                for i in range(tiles):
                    span = slice(i * tile, (i + 1) * tile)
                    v = rows_buf[e, rows, span].astype(f32)
                    rows_buf[e, rows, span] = (v * scale * gains[:, span]).astype(bf16)
            return carry

        lax.fori_loop(0, count // block, step, 0)

    def expand(e):
        def narrow(lo, size):
            up_in = rows_buf[e]
            gate = lax.dot_general(up_in, gbuf[2 * e, pl.ds(lo, size), :], last, preferred_element_type=f32)
            up = lax.dot_general(up_in, gbuf[2 * e + 1, pl.ds(lo, size), :], last, preferred_element_type=f32)
            inner[:, pl.ds(lo, size)] = (jax.nn.silu(gate) * up).astype(bf16)

        def step(n, carry):
            narrow(pl.multiple_of(n * 128, 128), 128)
            return carry

        lax.fori_loop(0, d_ff // 128, step, 0)
        if d_ff % 128:
            narrow(d_ff // 128 * 128, d_ff % 128)

    def y_copy(e, i, pos):
        return pltpu.make_async_remote_copy(
            src_ref=rows_buf.at[e, pl.ds(pos * cap, cap), cols(i)],
            dst_ref=ret.at[pl.ds(pl.multiple_of((me * local + e) * cap, cap), cap), cols(i)],
            send_sem=ysend.at[e, i], recv_sem=yrecv.at[e, i],
            device_id={'ep': peers[pos]}, device_id_type=MESH_ID,
        )

    def contract(e):
        def step(i, carry):
            q = e * tiles + i
            wd_copy(q).wait()
            y = jnp.dot(inner[...], wdbuf[lax.rem(q, wd_slots)], preferred_element_type=f32).astype(bf16)

            @pl.when(q + wd_slots < wd_total)
            def _():
                wd_copy(q + wd_slots).start()

            rows_buf[e, :, cols(i)] = y
            ret[pl.ds(pl.multiple_of((me * local + e) * cap, cap), cap), cols(i)] = y[:cap]
            for pos in range(1, n_ep):
                y_copy(e, i, pos).start()
            return carry

        lax.fori_loop(0, tiles, step, 0)

    lax.fori_loop(0, tiles, across, 0)
    lax.fori_loop(0, tiles, across2, 0)
    normalise(0, n_ep * cap)
    for g in range(2 * local):
        ff_copy(g).wait()

    def serve(e, carry):
        expand(e)
        contract(e)
        return carry

    lax.fori_loop(0, local, serve, 0)

    whole = pl.ds(0, (n_ep - 1) * cap)

    def finish(i, carry):
        for e in range(local):
            pltpu.make_async_copy(ret.at[whole, cols(i)], ret.at[whole, cols(i)], yrecv.at[e, i]).wait()
        picked = jnp.dot(comb[...], ret[:, cols(i)], preferred_element_type=f32)
        reps = tile // 128
        g0 = jnp.concatenate([gates[0]] * reps, axis=1)
        g1 = jnp.concatenate([gates[1]] * reps, axis=1)
        out[:, cols(i)] = xall[me, i].astype(f32) + (g0 * picked[:tokens] + g1 * picked[tokens:])
        return carry

    lax.fori_loop(0, tiles, finish, 0)

    def drain(i, carry):
        for kind in (0, 1, 2, 3, 4, 5, 6):
            pltpu.make_async_copy(xall.at[0, i], xall.at[0, i], xsend.at[kind, i]).wait()
        for e in range(local):
            pltpu.make_async_copy(ret.at[whole, cols(i)], ret.at[whole, cols(i)], ysend.at[e, i]).wait()
        return carry

    lax.fori_loop(0, tiles, drain, 0)
    pltpu.make_async_copy(sel_in.at[pl.ds(0, n_ep - 1)], sel_in.at[pl.ds(0, n_ep - 1)], sel_send).wait()


def moe(mix, hidden, expert_ids, ffn_gain, w_out, w_router, w_gate, w_up, w_down, n_ep):
    tokens, d_model = hidden.shape
    local, _, d_ff = w_gate.shape
    n_experts = local * n_ep
    cap = 4 * tokens // n_experts
    tile = 512
    tiles = d_model // tile
    vmem = pl.BlockSpec(memory_space=pltpu.VMEM)
    hbm = pl.BlockSpec(memory_space=pl.ANY)
    dma = pltpu.SemaphoreType.DMA
    return pl.pallas_call(
        functools.partial(moe_kernel, n_ep=n_ep, tile=tile, cap=cap),
        out_shape=jax.ShapeDtypeStruct((tokens, d_model), jnp.float32),
        in_specs=[vmem] * 5 + [hbm] * 4,
        out_specs=vmem,
        scratch_shapes=[
            pltpu.VMEM((2 * local, d_ff, d_model), jnp.bfloat16),
            pltpu.VMEM((4, d_ff, tile), jnp.bfloat16),
            pltpu.VMEM((n_ep, tiles, tokens, tile), jnp.bfloat16),
            pltpu.VMEM((local, n_ep * cap, d_model), jnp.bfloat16),
            pltpu.VMEM((n_ep * cap, d_ff), jnp.bfloat16),
            pltpu.VMEM((n_experts * cap, d_model), jnp.bfloat16),
            pltpu.VMEM((n_ep, local * cap, tokens), jnp.bfloat16),
            pltpu.VMEM((n_ep, local * cap, tokens), jnp.bfloat16),
            pltpu.VMEM((2 * tokens, n_experts * cap), jnp.bfloat16),
            pltpu.VMEM((2, tokens, 128), jnp.float32),
            pltpu.VMEM((1, d_model), jnp.float32),
            dma((4,)), dma((4,)), dma((4,)),
            dma((7, tiles)), dma((n_ep, tiles)),
            dma, dma,
            dma((local, tiles)), dma((local, tiles)),
        ],
        compiler_params=pltpu.CompilerParams(collective_id=0, has_side_effects=True, vmem_limit_bytes=VMEM_LIMIT),
        name="moe",
    )(mix, hidden, expert_ids.T, ffn_gain.reshape(-1, 128), w_router.T, w_out, w_gate.transpose(0, 2, 1), w_up.transpose(0, 2, 1), w_down)


def packed_kernel(
    mix, hidden, ids_row, gain, router, wo, wg, wu, wd,
    out, fits,
    gbuf, wdbuf, xown, xmate, stage, xin, rows_buf, wide_acc, inner, ret, ycross, ystage,
    slots_out, slots_in, spread, own_sel, sel, pack, comb, gates, gains, scale_out, scale_in, row_scale,
    wo_sem, wg_sem, wd_sem, slot_send, slot_recv, near_send, far_send, mate_send, fwd_send, x_recv, mate_recv,
    ysend_mate, yrecv_mate, cross_send, cross_recv, ysend, yrecv, scale_send, scale_recv, done, out_sem,
    *, n_ep, tile, cap, room,
):
    tokens, d_model = hidden.shape
    d_ff = wg.shape[1]
    local = wg.shape[0]
    n_experts = local * n_ep
    tiles = d_model // tile
    ring = n_ep // 2
    slab = local * cap
    chip_slab = 2 * slab
    f32, bf16 = jnp.float32, jnp.bfloat16
    last = (((1,), (1,)), ((), ()))

    me = lax.axis_index('ep')
    x, c = me // 2, lax.rem(me, 2)
    other = 1 - c

    def at(step, core):
        return lax.rem(x + step, ring) * 2 + core

    mate = at(0, other)
    places = [at(3, c), at(3, other), at(1, c), at(1, other), at(2, c), at(2, other)]
    peers = [mate] + places

    def cols(i):
        return pl.ds(pl.multiple_of(i * tile, tile), tile)

    def to(dev):
        return {'device_id': {'ep': dev}, 'device_id_type': MESH_ID}

    def landed(ref, sem):
        pltpu.make_async_copy(ref, ref, sem).wait()

    parts = d_model // tile

    def wo_start(i, slot):
        for j in range(parts):
            span = slice(j * tile, (j + 1) * tile)
            pltpu.make_async_copy(wo.at[span, cols(i)], gbuf.at[slot, 0:tile, span], wo_sem.at[slot]).start()

    def wo_wait(slot):
        pltpu.make_async_copy(wo.at[0:tile, :], gbuf.at[slot, 0:tile, :], wo_sem.at[slot]).wait()

    def ff_copy(g):
        src = wg if g % 2 == 0 else wu
        return pltpu.make_async_copy(src.at[g // 2], gbuf.at[g], wg_sem.at[g])

    wd_slots = wdbuf.shape[0]
    wd_total = local * tiles

    def tile_of(q):
        k = lax.rem(q // local, tiles)
        return 2 * (k // 2) + lax.rem(other + lax.rem(k, 2), 2)

    def wd_get(q):
        slot = lax.rem(q, wd_slots)
        return pltpu.make_async_copy(wd.at[lax.rem(q, local), :, cols(tile_of(q))], wdbuf.at[slot], wd_sem.at[slot])

    def wd_wait(q):
        wd_get(q).wait()

    def wd_next(q):
        @pl.when(q + wd_slots < wd_total)
        def _():
            wd_get(q + wd_slots).start()

    for i in range(4):
        wo_start(i, i)

    barrier = pltpu.get_barrier_semaphore()
    for peer in peers:
        pl.semaphore_signal(barrier, inc=1, device_id={'ep': peer}, device_id_type=MESH_ID)

    t_sub = lax.broadcasted_iota(jnp.int32, (tokens, tokens), 0)
    t_lane = lax.broadcasted_iota(jnp.int32, (tokens, tokens), 1)
    before = (t_sub < t_lane).astype(f32).astype(bf16)
    id0_row, id1_row = ids_row[0:1, :].astype(f32), ids_row[1:2, :].astype(f32)
    e_sub = lax.broadcasted_iota(jnp.int32, (n_experts, tokens), 0).astype(f32)
    spread_gain(gain, gains)
    hit_row = jnp.logical_or(e_sub == id0_row, e_sub == id1_row).astype(f32).astype(bf16)
    rank_row = jnp.dot(hit_row, before, preferred_element_type=f32)
    slots_row = []
    for ident in (id0_row, id1_row):
        rank = jnp.sum(jnp.where(e_sub == ident, rank_row, 0.0), axis=0, keepdims=True)
        slots_row.append(ident * cap + rank)
    eight = lax.broadcasted_iota(jnp.int32, (8, tokens), 0)
    slots_out[...] = jnp.where(eight == 0, slots_row[0], slots_row[1])

    def inside(slot, chip):
        low = (chip * chip_slab).astype(f32) if not isinstance(chip, int) else float(chip * chip_slab)
        return jnp.logical_and(slot >= low, slot < low + chip_slab).astype(f32)

    def ranks(s0, s1, chip):
        in0, in1 = inside(s0, chip), inside(s1, chip)
        uses = jnp.maximum(in0, in1)
        rows = jnp.where(eight == 0, uses, jnp.where(eight == 1, in0, in1))
        got = jnp.dot(rows.astype(bf16), before, preferred_element_type=f32)
        base = jnp.sum(in0, axis=1, keepdims=True)
        return in0, in1, uses, got[0:1, :], got[1:2, :], base + got[2:3, :]

    p_sub = lax.broadcasted_iota(jnp.int32, (room, tokens), 0).astype(f32)
    steps = (3, 1, 2)
    index = [jnp.zeros((1, tokens), f32), jnp.zeros((1, tokens), f32)]
    for k, step in enumerate(steps):
        in0, in1, uses, dpos, q0, q1 = ranks(slots_row[0], slots_row[1], lax.rem(x + step, ring))
        spread[k] = jnp.logical_and(p_sub == dpos, uses > 0.5).astype(f32).astype(bf16)
        index[0] = index[0] + in0 * (k * room + q0)
        index[1] = index[1] + in1 * (k * room + q1)
    mine_low = (x * chip_slab).astype(f32)
    for k in range(2):
        index[k] = index[k] + inside(slots_row[k], x) * (3 * room + slots_row[k] - mine_low)
    def slot_sel(dev, s0, s1):
        want = (lax.broadcasted_iota(jnp.int32, (slab, tokens), 0) + dev * slab).astype(f32)
        return jnp.logical_or(want == s0, want == s1).astype(f32).astype(bf16)

    pl.semaphore_wait(barrier, n_ep - 1)
    for k, peer in enumerate(peers):
        there = (0, 3, 4, 1, 2, 5, 6)[k]
        pltpu.make_async_remote_copy(
            src_ref=slots_out, dst_ref=slots_in.at[there], send_sem=slot_send.at[k], recv_sem=slot_recv.at[there], **to(peer),
        ).start()

    def x_copy(place, i):
        k, dev, there = {0: (0, places[0], 2), 2: (1, places[2], 0), 4: (2, places[4], 4)}[place]
        sem = near_send.at[k, i] if k < 2 else far_send.at[i]
        return pltpu.make_async_remote_copy(
            src_ref=stage.at[k, i], dst_ref=xin.at[there, i], send_sem=sem, recv_sem=x_recv.at[there, i], **to(dev),
        )

    def mate_copy(i):
        return pltpu.make_async_remote_copy(
            src_ref=xown.at[i], dst_ref=xmate.at[i], send_sem=mate_send.at[i], recv_sem=mate_recv.at[i], **to(mate),
        )

    def fwd_copy(place, i):
        return pltpu.make_async_remote_copy(
            src_ref=xin.at[place, i], dst_ref=xin.at[place + 1, i], send_sem=fwd_send.at[place // 2, i],
            recv_sem=x_recv.at[place + 1, i], **to(mate),
        )

    own_sel[0] = slot_sel(me, slots_row[0], slots_row[1])
    c_lane = lax.broadcasted_iota(jnp.int32, (chip_slab, tokens), 0)
    want = (lax.rem(c_lane + c * slab, chip_slab) + x * chip_slab).astype(f32)

    def learn(k):
        landed(slots_in.at[k], slot_recv.at[k])
        s0, s1 = slots_in[k, 0:1, :], slots_in[k, 1:2, :]
        own_sel[k + 1] = slot_sel(me, s0, s1)
        in0, in1, uses, dpos, q0, q1 = ranks(s0, s1, x)
        put = jnp.logical_and(p_sub == dpos, uses > 0.5).astype(f32).astype(bf16)
        sel[k] = lax.dot_general(own_sel[k + 1], put, last, preferred_element_type=f32).astype(bf16)
        total = jnp.zeros((room, chip_slab), f32)
        for s, inn, q in ((s0, in0, q0), (s1, in1, q1)):
            spot = jnp.logical_and(p_sub == q, inn > 0.5).astype(f32).astype(bf16)
            total = total + lax.dot_general(spot, (want == s).astype(f32).astype(bf16), last, preferred_element_type=f32)
        pack[k] = total.astype(bf16)

    early = 5

    def project(i, carry):
        slot = lax.rem(i, 4)
        wo_wait(slot)
        acc = jnp.zeros((tokens, tile), f32)
        for j in range(parts):
            span = slice(j * tile, (j + 1) * tile)
            acc = acc + jnp.dot(mix[:, span], gbuf[slot, 0:tile, span], preferred_element_type=f32)
        xt = (hidden[:, cols(i)].astype(f32) + acc).astype(bf16)
        xown[i] = xt
        for k in range(3):
            stage[k, i] = jnp.dot(spread[k], xt, preferred_element_type=f32).astype(bf16)
        @pl.when(i < early)
        def _():
            x_copy(0, i).start()
            x_copy(2, i).start()

        mate_copy(i).start()

        wide = xt.astype(f32)
        wide = wide * wide
        for j in range(0, tile, 128):
            carry = carry + wide[:, j:j + 128]

        @pl.when(i < 4)
        def _():
            wo_start(i + 4, slot)

        for g in range(4):
            @pl.when(i == g + 4)
            def _():
                ff_copy(g).start()
        return carry

    sums = lax.fori_loop(0, tiles, project, jnp.zeros((tokens, 128), f32))
    inv = lax.rsqrt(jnp.sum(sums, axis=1, keepdims=True) / d_model + NORM_EPS)
    inv_row = jnp.broadcast_to(inv, (tokens, 128)).T[0:8, :]
    scale_out[...] = inv_row
    for k, peer in enumerate(peers):
        there = (0, 3, 4, 1, 2, 5, 6)[k]
        pltpu.make_async_remote_copy(
            src_ref=scale_out, dst_ref=scale_in.at[there], send_sem=scale_send.at[k], recv_sem=scale_recv.at[there], **to(peer),
        ).start()

    def send_near(i, carry):
        x_copy(0, i).start()
        x_copy(2, i).start()
        return carry

    lax.fori_loop(early, tiles, send_near, 0)

    def send_far(i, carry):
        x_copy(4, i).start()
        return carry

    lax.fori_loop(0, tiles, send_far, 0)
    for k in range(n_ep - 1):
        learn(k)
    for q in range(wd_slots):
        wd_get(jnp.int32(q)).start()

    def learn_scale(k, row):
        hit = own_sel[k].astype(f32) * row
        row_scale[k] = jnp.broadcast_to(jnp.sum(hit, axis=1, keepdims=True), (slab, 128))

    def gather(pick, block, pos, i):
        got = jnp.dot(pick, block, preferred_element_type=f32)
        mul = jnp.concatenate([row_scale[pos]] * (tile // 128), axis=1)
        got = (got * mul * gains[:, cols(i)]).astype(bf16)
        for e in range(local):
            rows_buf[e, pos * cap:(pos + 1) * cap, cols(i)] = got[e * cap:(e + 1) * cap]

    def scale_from(k):
        landed(scale_in.at[k], scale_recv.at[k])
        learn_scale(k + 1, scale_in[k, 0:1, :])

    learn_scale(0, inv_row[0:1, :])
    for k in range(5):
        scale_from(k)

    def near_rows(i):
        for place in (1, 3):
            landed(xin.at[place, i], x_recv.at[place, i])
        for place in range(4):
            gather(sel[place + 1], xin[place, i], place + 2, i)

    def own(i, carry):
        for place in (0, 2):
            landed(xin.at[place, i], x_recv.at[place, i])
            fwd_copy(place, i).start()
        landed(xmate.at[i], mate_recv.at[i])
        gather(own_sel[0], xown[i], 0, i)
        gather(own_sel[1], xmate[i], 1, i)

        @pl.when(i > 0)
        def _():
            near_rows(i - 1)
        return carry

    lax.fori_loop(0, tiles, own, 0)
    near_rows(tiles - 1)
    for k in range(5, 7):
        scale_from(k)

    for g in range(2 * local):
        ff_copy(g).wait()

    def expand(i):
        for e in range(local):
            for k in range(2):
                part = lax.dot_general(rows_buf[e, :, cols(i)], gbuf[2 * e + k, :, cols(i)], last, preferred_element_type=f32)
                wide_acc[2 * e + k] = jnp.where(i == 0, part, wide_acc[2 * e + k] + part)

    def last_source(i):
        landed(xin.at[5, i], x_recv.at[5, i])
        gather(sel[6], xin[5, i], 7, i)
        expand(i)

    def across(i, carry):
        landed(xin.at[4, i], x_recv.at[4, i])
        fwd_copy(4, i).start()
        gather(sel[5], xin[4, i], 6, i)

        @pl.when(i > 0)
        def _():
            last_source(i - 1)
        return carry

    lax.fori_loop(0, tiles, across, 0)
    last_source(tiles - 1)
    for e in range(local):
        inner[e] = (jax.nn.silu(wide_acc[2 * e]) * wide_acc[2 * e + 1]).astype(bf16)


    def mate_y(e, i):
        return pltpu.make_async_remote_copy(
            src_ref=rows_buf.at[e, pl.ds(cap, cap), cols(i)],
            dst_ref=ret.at[pl.ds(pl.multiple_of(3 * room + c * slab + e * cap, cap // 2), cap), cols(i)],
            send_sem=ysend_mate.at[e, i], recv_sem=yrecv_mate.at[e, i], **to(mate),
        )

    lead = 2 * cap

    def cross_y(e, i):
        rows = pl.ds(lead, n_ep * cap - lead)
        return pltpu.make_async_remote_copy(
            src_ref=rows_buf.at[e, rows, cols(i)], dst_ref=ycross.at[i // 2, e, rows],
            send_sem=cross_send.at[e, i // 2], recv_sem=cross_recv.at[e, i // 2], **to(mate),
        )

    def y_copy(place, half, i):
        there = (1, 1, 0, 0, 2, 2)[place]
        return pltpu.make_async_remote_copy(
            src_ref=ystage.at[place, half], dst_ref=ret.at[pl.ds(there * room, room), cols(i)],
            send_sem=ysend.at[place, half], recv_sem=yrecv.at[there, i], **to(places[place]),
        )

    def contract():
        def finish_pair(half):
            i = 2 * half + c
            for e in range(local):
                landed(ycross.at[half, e, pl.ds(lead, n_ep * cap - lead)], cross_recv.at[e, half])
            for pos in (6, 7, 2, 3, 4, 5):
                block_rows = slice(pos * cap, (pos + 1) * cap)
                swapped = slice((pos ^ 1) * cap, ((pos ^ 1) + 1) * cap)
                pieces = [rows_buf[e, block_rows, cols(i)] for e in range(local)] + [ycross[half, e, swapped, :] for e in range(local)]
                ystage[pos - 2, half] = jnp.dot(pack[pos - 1], jnp.concatenate(pieces, axis=0), preferred_element_type=f32).astype(bf16)
                y_copy(pos - 2, half, i).start()

        def pair(half, carry):
            for k in range(2):
                i = 2 * half + (lax.rem(other + k, 2))
                for e in range(local):
                    q = (2 * half + k) * local + e
                    wd_wait(q)
                    y = jnp.dot(inner[e], wdbuf[lax.rem(q, wd_slots)], preferred_element_type=f32).astype(bf16)
                    wd_next(q)
                    rows_buf[e, :, cols(i)] = y
                    if k == 0:
                        cross_y(e, i).start()
                    ret[pl.ds(pl.multiple_of(3 * room + c * slab + e * cap, cap // 2), cap), cols(i)] = y[:cap]
                    mate_y(e, i).start()
            finish_pair(half)
            return carry

        lax.fori_loop(0, tiles // 2, pair, 0)

    contract()

    width = 3 * room + chip_slab
    w_lane = lax.broadcasted_iota(jnp.int32, (tokens, width), 1).astype(f32)
    for k in range(2):
        comb[k * tokens:(k + 1) * tokens, :] = (w_lane == column_of(index[k])[:, 0:1]).astype(f32).astype(bf16)

    top = jnp.zeros((1, 1), f32)
    for s0, s1 in [(slots_row[0], slots_row[1])] + [(slots_in[k, 0:1, :], slots_in[k, 1:2, :]) for k in range(n_ep - 1)]:
        for d in range(ring):
            top = jnp.maximum(top, jnp.sum(inside(s0, d) + inside(s1, d), axis=1, keepdims=True))
    fits[0] = (top[0, 0] <= room).astype(jnp.int32)

    def route(i, acc):
        v = (xown[i].astype(f32) * inv * gains[:, cols(i)]).astype(bf16)
        return acc + lax.dot_general(v, router[:, cols(i)], last, preferred_element_type=f32)

    logits = lax.fori_loop(0, tiles, route, jnp.zeros((tokens, n_experts), f32))
    e_lane = lax.broadcasted_iota(jnp.int32, (tokens, n_experts), 1).astype(f32)
    id0, id1 = column_of(id0_row)[:, 0:1], column_of(id1_row)[:, 0:1]
    l0 = jnp.sum(jnp.where(e_lane == id0, logits, 0.0), axis=1, keepdims=True)
    l1 = jnp.sum(jnp.where(e_lane == id1, logits, 0.0), axis=1, keepdims=True)
    top = jnp.maximum(l0, l1)
    e0, e1 = jnp.exp(l0 - top), jnp.exp(l1 - top)
    gates[0] = jnp.broadcast_to(e0 / (e0 + e1), (tokens, 128))
    gates[1] = jnp.broadcast_to(e1 / (e0 + e1), (tokens, 128))

    def finish(i, carry):
        for e in range(local):
            landed(ret.at[pl.ds(0, cap), cols(i)], yrecv_mate.at[e, i])
        for k in range(3):
            landed(ret.at[pl.ds(0, room), cols(i)], yrecv.at[k, i])
        picked = jnp.dot(comb[...], ret[:, cols(i)], preferred_element_type=f32)
        reps = tile // 128
        g0 = jnp.concatenate([gates[0]] * reps, axis=1)
        g1 = jnp.concatenate([gates[1]] * reps, axis=1)
        done[i] = xown[i].astype(f32) + (g0 * picked[:tokens] + g1 * picked[tokens:])
        pltpu.make_async_copy(done.at[i], out.at[:, cols(i)], out_sem.at[i]).start()
        return carry

    lax.fori_loop(0, tiles, finish, 0)

    def drain(i, carry):
        for k in range(2):
            landed(stage.at[0, 0], near_send.at[k, i])
        landed(stage.at[0, 0], far_send.at[i])
        landed(xown.at[0], mate_send.at[i])
        pltpu.make_async_copy(done.at[i], out.at[:, cols(i)], out_sem.at[i]).wait()
        for k in range(3):
            landed(stage.at[0, 0], fwd_send.at[k, i])
        for e in range(local):
            landed(ret.at[pl.ds(0, cap), cols(0)], ysend_mate.at[e, i])
        return carry

    lax.fori_loop(0, tiles, drain, 0)

    def drain2(half, carry):
        for e in range(local):
            landed(ycross.at[0, 0, pl.ds(lead, n_ep * cap - lead)], cross_send.at[e, half])
        for place in range(6):
            landed(ystage.at[0, 0], ysend.at[place, half])
        return carry

    lax.fori_loop(0, tiles // 2, drain2, 0)
    for k in range(7):
        landed(slots_out, slot_send.at[k])
        landed(scale_out, scale_send.at[k])


def moe_packed(mix, hidden, expert_ids, ffn_gain, w_out, w_router, w_gate, w_up, w_down, n_ep, room):
    tokens, d_model = hidden.shape
    local, _, d_ff = w_gate.shape
    n_experts = local * n_ep
    cap = 4 * tokens // n_experts
    slab = local * cap
    tile = 512
    tiles = d_model // tile
    vmem = pl.BlockSpec(memory_space=pltpu.VMEM)
    hbm = pl.BlockSpec(memory_space=pl.ANY)
    dma = pltpu.SemaphoreType.DMA
    bf16 = jnp.bfloat16
    return pl.pallas_call(
        functools.partial(packed_kernel, n_ep=n_ep, tile=tile, cap=cap, room=room),
        out_shape=(jax.ShapeDtypeStruct((tokens, d_model), jnp.float32), jax.ShapeDtypeStruct((1,), jnp.int32)),
        in_specs=[vmem] * 5 + [hbm] * 4,
        out_specs=(hbm, pl.BlockSpec(memory_space=pltpu.SMEM)),
        scratch_shapes=[
            pltpu.VMEM((2 * local, d_ff, d_model), bf16),
            pltpu.VMEM((4, d_ff, tile), bf16),
            pltpu.VMEM((tiles, tokens, tile), bf16),
            pltpu.VMEM((tiles, tokens, tile), bf16),
            pltpu.VMEM((3, tiles, room, tile), bf16),
            pltpu.VMEM((6, tiles, room, tile), bf16),
            pltpu.VMEM((local, n_ep * cap, d_model), bf16),
            pltpu.VMEM((2 * local, n_ep * cap, d_ff), jnp.float32),
            pltpu.VMEM((local, n_ep * cap, d_ff), bf16),
            pltpu.VMEM((3 * room + 2 * slab, d_model), bf16),
            pltpu.VMEM((tiles // 2, local, n_ep * cap, tile), bf16),
            pltpu.VMEM((6, tiles // 2, room, tile), bf16),
            pltpu.VMEM((8, tokens), jnp.float32),
            pltpu.VMEM((7, 8, tokens), jnp.float32),
            pltpu.VMEM((3, room, tokens), bf16),
            pltpu.VMEM((n_ep, slab, tokens), bf16),
            pltpu.VMEM((n_ep - 1, slab, room), bf16),
            pltpu.VMEM((n_ep - 1, room, 2 * slab), bf16),
            pltpu.VMEM((2 * tokens, 3 * room + 2 * slab), bf16),
            pltpu.VMEM((2, tokens, 128), jnp.float32),
            pltpu.VMEM((1, d_model), jnp.float32),
            pltpu.VMEM((8, tokens), jnp.float32),
            pltpu.VMEM((n_ep - 1, 8, tokens), jnp.float32),
            pltpu.VMEM((n_ep, slab, 128), jnp.float32),
            dma((4,)), dma((4,)), dma((4,)),
            dma((7,)), dma((7,)),
            dma((2, tiles)), dma((tiles,)), dma((tiles,)), dma((3, tiles)), dma((6, tiles)), dma((tiles,)),
            dma((local, tiles)), dma((local, tiles)),
            dma((local, tiles // 2)), dma((local, tiles // 2)),
            dma((6, tiles // 2)), dma((3, tiles)),
            dma((n_ep - 1,)), dma((n_ep - 1,)),
            pltpu.VMEM((tiles, tokens, tile), jnp.float32), dma((tiles,)),
        ],
        compiler_params=pltpu.CompilerParams(collective_id=1, has_side_effects=True, vmem_limit_bytes=VMEM_LIMIT),
        name="moe_packed",
    )(mix, hidden, expert_ids.T, ffn_gain.reshape(-1, 128), w_router.T, w_out, w_gate.transpose(0, 2, 1), w_up.transpose(0, 2, 1), w_down)


def solution(mesh):
    n_ep = mesh.shape['ep']
    row_spec = P(('dp', 'ep'), None)
    cache_spec = P(('dp', 'ep'), None, None, None)
    expert_spec = P('ep', None, None)
    in_specs = (row_spec, cache_spec, cache_spec, P(('dp', 'ep')), row_spec, P(), P(), P(), P(), P(), P(), P(), expert_spec, expert_spec, expert_spec)
    out_specs = (row_spec, cache_spec, cache_spec)

    def device_step(hidden, k_cache, v_cache, seq_lens, expert_ids, attn_gain, w_query, w_key, w_value, w_out, ffn_gain, w_router, w_gate, w_up, w_down):
        mix, k_cache_new, v_cache_new = attention(hidden, k_cache, v_cache, seq_lens, attn_gain, w_query, w_key, w_value)
        operands = (mix, hidden, expert_ids, ffn_gain, w_out, w_router, w_gate, w_up, w_down)
        room = 5 * hidden.shape[0] // 8
        out, fits = moe_packed(*operands, n_ep, room)
        out = lax.cond(fits[0] == 1, lambda ops: ops[0].astype(jnp.bfloat16), lambda ops: moe(*ops[1:], n_ep).astype(jnp.bfloat16), (out,) + operands)
        return out, k_cache_new, v_cache_new

    return jax.shard_map(device_step, mesh=mesh, in_specs=in_specs, out_specs=out_specs, check_vma=False)
```
